256 devices in a mesh: wave: 32 (over z, x_hi, core), lev: 8 (over y, x_lo).
Axes of the slice: x: 4 (x_hi: 2, x_lo: 2; x = x_hi * 2 + x_lo), y: 4, z: 8, core: 2. Of those that a mesh axis runs over, the one named last changes fastest.
Arguments:
- spectral: float32 [136, 1024, 2562], P('lev', 'wave'), may hold values from -6 to 6
- to_modes: float32 [136, 136], replicated, may hold values from -3 to 3
- from_modes: float32 [136, 136], replicated, may hold values from -3 to 3
- depth: float32 [136], replicated, may hold values from 0.02 to 50
- owner: int32 [512], replicated, may hold values from 0 to 31, as said below
Outputs:
- solved: float32 [136, 512, 2562], P('lev', 'wave')
The draws below stay inside these ranges and needn't reach their ends.
Inputs may be any that keep to these rules, and one draw needn't show every extreme that they name: `owner`: group q holds the pairs q * 1 to q * 1 + 1 - 1; a device stores its groups in increasing q from its first slot on, 1 slots each, and leaves its other slots unused. The 16 groups with the same q // 16 have 16 different owners. A device owns at most 32 groups, and some device exactly that many.
All inputs are finite; a program needn't handle non-finite values.
Results may differ from the reference program's by a relative error of at most 0.000075.
Values sent between devices are 32-bit elements; how exact they have to be, the bound alone decides.
A program may use at most 128 MiB of HBM per device.

```python
import math
import jax
import jax.numpy as jnp
from jax import lax

NT = 1279
LEVELS = 136
KPAIR = 1
GROUPS = 16
PLEN = 1281
CAP = 32
PAIRS = 512
SLOTS = 1024
NGROUPS = 512
N_WAVE = 32


def modes_matrix(key, salt):
    base = jax.random.fold_in(key, salt)
    first = jax.random.fold_in(base, 0)
    noise = jnp.clip(jax.random.normal(first, (LEVELS, LEVELS), jnp.float32), -4.0, 4.0)
    matrix = jnp.eye(LEVELS, dtype=jnp.float32) + 0.5 * noise / math.sqrt(LEVELS)
    return matrix


def draw_to_modes(key, part):
    return modes_matrix(key, 31)


def draw_from_modes(key, part):
    return modes_matrix(key, 47)


def draw_owner(key, part):
    first, second = jax.random.split(jax.random.fold_in(key, 11))
    half = N_WAVE // 2
    shifts = jax.random.randint(first, (half,), 0, GROUPS + 1).astype(jnp.int32)
    shifts = shifts.at[0].set(GROUPS)
    counts = jnp.concatenate([GROUPS + shifts, GROUPS - shifts])
    labels = jax.random.permutation(second, N_WAVE).astype(jnp.int32)
    bounds = jnp.cumsum(counts)
    positions = jnp.arange(NGROUPS, dtype=jnp.int32)
    runs = jnp.sum((positions[:, None] >= bounds[None, :]).astype(jnp.int32), axis=1)
    sequence = labels[runs]
    target = positions // GROUPS
    within = positions % GROUPS
    return sequence[within * N_WAVE + target].astype(jnp.int32)


def level_of(stream_key, dims, pieces, low, largest):
    factor_of, own = 1.0, jax.random.fold_in(stream_key, 6)
    for axis_at, parts in pieces:
        steps = jnp.exp(jax.random.uniform(jax.random.fold_in(own, axis_at), (parts,), jnp.float32, low / len(pieces), largest / len(pieces)))
        factor_of = factor_of * jnp.repeat(steps, dims[axis_at] // parts).reshape([-1 if axis == axis_at else 1 for axis in range(len(dims))])
    return factor_of


def scatter_about(own_key, shape, scale, bound, shards=(), kind=jnp.bfloat16):
    result = scale * jax.random.normal(own_key, shape, jnp.float32)
    if shards:
        result = result * level_of(own_key, shape, shards, -0.22, 0.18)
    return jnp.clip(result, -bound, bound).astype(kind)


def setup_inputs(seed: int = 0) -> dict:
    seeds = jax.random.split(jax.random.key(seed), 6)
    return {
        "spectral": scatter_about(seeds[0], (LEVELS, SLOTS, 2 * PLEN), 1.0, 6.0, ((0, 8), (1, 32)), jnp.float32),
        "to_modes": draw_to_modes(jax.random.fold_in(seeds[5], 71), 0),
        "from_modes": draw_from_modes(jax.random.fold_in(seeds[5], 71), 0),
        "depth": jnp.clip(jnp.exp(jax.random.uniform(seeds[3], (LEVELS,), jnp.float32, math.log(0.02), math.log(50.0))), 0.02, 50.0),
        "owner": draw_owner(jax.random.fold_in(seeds[5], 71), 0),
    }


def reference(spectral, to_modes, from_modes, depth, owner):
    numbers = jnp.arange(NGROUPS, dtype=jnp.int32)
    same = owner[:, None] == owner[None, :]
    rank = jnp.sum((same & (numbers[None, :] < numbers[:, None])).astype(jnp.int32), axis=1)
    first = owner * CAP + rank * KPAIR
    source = (first[:, None] + jnp.arange(KPAIR, dtype=jnp.int32)[None, :]).reshape(PAIRS).astype(jnp.int32)
    moved = jnp.take(spectral, source, axis=1)
    flat = moved.reshape(LEVELS, PAIRS * 2 * PLEN)
    pair = jnp.arange(PAIRS, dtype=jnp.int32)[:, None]
    column = jnp.arange(2 * PLEN, dtype=jnp.int32)[None, :]
    within = column % PLEN
    degree = jnp.where(within <= NT - pair, pair + within, within - 1)
    ratio = (degree * (degree + 1)).astype(jnp.float32) / float(NT * (NT + 1))
    ratio = ratio.reshape(PAIRS * 2 * PLEN)
    modes = jnp.dot(to_modes, flat, precision=lax.Precision.HIGHEST, preferred_element_type=jnp.float32)
    scaled = modes / (1.0 + depth[:, None] * ratio[None, :])
    solved = jnp.dot(from_modes, scaled, precision=lax.Precision.HIGHEST, preferred_element_type=jnp.float32)
    return solved.reshape(LEVELS, PAIRS, 2 * PLEN)
```

```python
import functools

import jax
import jax.numpy as jnp
from jax import lax
from jax.experimental import pallas as pl
from jax.experimental.pallas import tpu as pltpu
from jax.sharding import PartitionSpec as P

NT = 1279
PLEN = NT + 2
LANES = 128
SIZES = (8, 8, 4)
MESH = pl.DeviceIdType.MESH


def rows_of(levels, tiles, rest):
    return -(-(levels * tiles + (rest > 0)) // 8) * 8


def kernel(
    waves, levs, number, levels, slots, rest, chunks,
    picks, senders, spectral, edge, to_modes, from_modes, depth, out, edge_out,
    held, result, matrix, packs, lands, picked, blocks, backs, homes,
    in_sem, out_sem, send1, recv1, send2, recv2, send3, recv3,
):
    me = lax.axis_index("wave")
    lev = lax.axis_index("lev")
    per = number // levs
    n = len(chunks)
    last = n - 1

    def load(c, t):
        at = chunks[c][0] + t
        return pltpu.make_async_copy(
            spectral.at[:, pl.ds(at * LANES, LANES)], held[c].at[t], in_sem.at[at]
        )

    def store(c, t):
        at = chunks[c][0] + t
        return pltpu.make_async_copy(
            result.at[at], out.at[:, pl.ds(at * LANES, LANES)], out_sem.at[at]
        )

    def each_tile(c, act):
        for t in range(chunks[c][1]):
            act(c, t)

    def wave_copy(c, k, at=None):
        peer = lax.rem(me + k, waves)
        at = me if at is None else peer
        return pltpu.make_async_remote_copy(
            src_ref=packs[c].at[peer], dst_ref=lands[c].at[at],
            send_sem=send1.at[c, peer], recv_sem=recv1.at[c, at],
            device_id={"wave": peer}, device_id_type=MESH,
        )

    def place(ref, c, at):
        if len(ref.shape) > 2:
            return ref.at[at]
        size = per * chunks[c][2]
        return ref.at[pl.ds(pl.multiple_of(at * size, 8), size)]

    def lev_copy(source, target, send, recv, c, peer, at):
        return pltpu.make_async_remote_copy(
            src_ref=place(source[c], c, peer), dst_ref=place(target[c], c, at),
            send_sem=send.at[c, peer], recv_sem=recv.at[c, at],
            device_id={"lev": peer}, device_id_type=MESH,
        )

    def modal(c, peer, at):
        return lev_copy(picked, blocks, send2, recv2, c, peer, at)

    def back(c, peer, at):
        return lev_copy(backs, homes, send3, recv3, c, peer, at)

    def gather(c):
        tiles = chunks[c][1]

        @pl.loop(0, waves)
        def _(d):
            slot = picks[d]
            for t in range(tiles):
                packs[c][d, pl.ds(t, levels, stride=tiles), :] = held[c][
                    t, pl.ds(slot, levels, stride=slots), :
                ]
            if c == last and rest:
                packs[c][d, pl.ds(levels * tiles, 1), :] = edge[pl.ds(slot, 1), :]

    def each_wave(act):
        pl.loop(1, waves)(act)

    def each_lev(act):
        pl.loop(1, levs)(lambda k: act(lax.rem(lev + k, levs)))

    def select(c):
        @pl.loop(0, number)
        def _(i):
            picked[c][i // per, lax.rem(i, per)] = lands[c][senders[i]]

        blocks[c][lev] = picked[c][lev]

    def solve(c):
        start, tiles, size = chunks[c]
        extra = c == last and rest > 0
        wide = (tiles + extra) * LANES
        row = lax.broadcasted_iota(jnp.int32, (levels, LANES), 0)
        lane = lax.broadcasted_iota(jnp.int32, (levels, LANES), 1)
        belongs = lane // max(rest, 1) == row
        first = lax.broadcasted_iota(jnp.int32, (LANES, LANES), 0)
        second = lax.broadcasted_iota(jnp.int32, (LANES, LANES), 1)

        def exact(a, b):
            return jnp.dot(
                a, b, precision=lax.Precision.HIGHEST, preferred_element_type=jnp.float32
            )

        @pl.loop(0, per)
        def _(p):
            for b in range(levs):
                rows = pl.ds(b * levels, levels)
                for t in range(tiles):
                    matrix[rows, pl.ds(t * LANES, LANES)] = blocks[c][
                        b, p, pl.ds(t, levels, stride=tiles), :
                    ]
                if extra:
                    line = blocks[c][b, p, pl.ds(levels * tiles, 1), :]
                    matrix[rows, pl.ds(tiles * LANES, LANES)] = jnp.where(belongs, line, 0.0)
            if extra:
                fold = (first % rest == second) & (first < levels * rest)
                edges = pl.ds(tiles * LANES, LANES)
                matrix[:, edges] = exact(matrix[:, edges], fold.astype(jnp.float32))
            modes = exact(to_modes[...], matrix[:, pl.ds(0, wide)])
            column = start * LANES + lax.broadcasted_iota(jnp.int32, (1, wide), 1)
            within = jnp.where(column >= PLEN, column - PLEN, column)
            pair = me * number + lev * per + p
            degree = jnp.where(within <= NT - pair, pair + within, within - 1)
            ratio = (degree * (degree + 1)).astype(jnp.float32) / float(NT * (NT + 1))
            scaled = modes / (1.0 + depth[...] * ratio)
            matrix[:, pl.ds(0, wide)] = exact(from_modes[...], scaled)
            if extra:
                spread = (second % rest == first) & (second < levels * rest)
                edges = pl.ds(tiles * LANES, LANES)
                matrix[:, edges] = exact(matrix[:, edges], spread.astype(jnp.float32))
            for b in range(levs):
                rows = pl.ds(b * levels, levels)
                base = (b * per + p) * size
                for t in range(tiles):
                    backs[c][pl.ds(base + t, levels, stride=tiles), :] = matrix[
                        rows, pl.ds(t * LANES, LANES)
                    ]
                if extra:
                    line = jnp.where(belongs, matrix[rows, pl.ds(tiles * LANES, LANES)], 0.0)
                    backs[c][pl.ds(base + levels * tiles, 1), :] = jnp.sum(
                        line, axis=0, keepdims=True
                    )

        own = pl.ds(pl.multiple_of(lev * per * size, 8), per * size)
        homes[c][own] = backs[c][own]

    def unpack(c):
        start, tiles, size = chunks[c]

        @pl.loop(0, levels)
        def _(l):
            rows = pl.ds(pl.multiple_of(l * number, number), number)
            for t in range(tiles):
                result[start + t, rows, :] = homes[c][pl.ds(l * tiles + t, number, stride=size), :]

        if c == last and rest:
            edge_out[...] = homes[c][pl.ds(levels * tiles, number, stride=size), :]

    for c in range(n):
        each_tile(c, lambda c, t: load(c, t).start())
    barrier = pltpu.get_barrier_semaphore()

    @pl.loop(1, waves)
    def _(k):
        pl.semaphore_signal(
            barrier, inc=1, device_id={"wave": lax.rem(me + k, waves)}, device_id_type=MESH
        )

    @pl.loop(1, levs)
    def _(k):
        pl.semaphore_signal(
            barrier, inc=1, device_id={"lev": lax.rem(lev + k, levs)}, device_id_type=MESH
        )

    each_tile(0, lambda c, t: load(c, t).wait())
    gather(0)
    pl.semaphore_wait(barrier, waves + levs - 2)
    each_wave(lambda k: wave_copy(0, k).start())
    lands[0][me] = packs[0][me]
    for c in range(1, n):
        each_tile(c, lambda c, t: load(c, t).wait())
        gather(c)
        lands[c][me] = packs[c][me]

    for c in range(n):
        if c < last:

            def follow(k, c=c):
                wave_copy(c, k).wait_send()
                wave_copy(c + 1, k).start()

            each_wave(follow)
        else:
            each_wave(lambda k, c=c: wave_copy(c, k).wait_send())
        each_wave(lambda k, c=c: wave_copy(c, k, True).wait_recv())
        select(c)
        each_lev(lambda j, c=c: modal(c, j, lev).start())
        each_lev(lambda j, c=c: modal(c, j, j).wait_recv())
        solve(c)
        each_lev(lambda j, c=c: back(c, j, lev).start())
        if c > 0:
            each_lev(lambda j, c=c: back(c - 1, j, j).wait_recv())
            unpack(c - 1)
            each_tile(c - 1, lambda c, t: store(c, t).start())
    each_lev(lambda j: back(last, j, j).wait_recv())
    unpack(last)
    each_tile(last, lambda c, t: store(c, t).start())
    for c in range(n):
        each_lev(lambda j, c=c: modal(c, j, j).wait_send())
        each_lev(lambda j, c=c: back(c, j, j).wait_send())
        each_tile(c, lambda c, t: store(c, t).wait())


def per_device(waves, levs, spectral, to_modes, from_modes, depth, owner):
    levels, slots, width = spectral.shape
    number = owner.shape[0] // waves
    per = number // levs
    me = lax.axis_index("wave")
    mine = jnp.sum((owner.reshape(waves, number) == me).astype(jnp.int32), axis=1)
    order = jnp.arange(waves, dtype=jnp.int32)
    before = jnp.where(order[None, :] < order[:, None], mine[None, :], 0)
    picks = jnp.minimum(jnp.sum(before, axis=1), slots - 1)
    senders = lax.dynamic_slice_in_dim(owner, me * number, number)

    tiles, rest = divmod(width, LANES)
    edge = spectral[:, :, tiles * LANES :].transpose(1, 0, 2).reshape(slots, levels * rest)
    edge = jnp.pad(edge, ((0, 0), (0, LANES - levels * rest)))
    n = len(SIZES)
    chunks = []
    for c, size in enumerate(SIZES):
        start = sum(SIZES[:c])
        chunks.append((start, size, rows_of(levels, size, rest if c == n - 1 else 0)))
    largest = max(SIZES) * LANES

    def buffers(*lead):
        return [pltpu.VMEM((*lead, r, LANES), jnp.float32) for _, _, r in chunks]

    flat = [pltpu.VMEM((number * r, LANES), jnp.float32) for _, _, r in chunks]
    vmem = pl.BlockSpec(memory_space=pltpu.VMEM)
    smem = pl.BlockSpec(memory_space=pltpu.SMEM)
    hbm = pl.BlockSpec(memory_space=pl.ANY)
    dma = pltpu.SemaphoreType.DMA
    body, side = pl.pallas_call(
        functools.partial(kernel, waves, levs, number, levels, slots, rest, chunks),
        out_shape=(
            jax.ShapeDtypeStruct((levels * number, tiles * LANES), jnp.float32),
            jax.ShapeDtypeStruct((number, LANES), jnp.float32),
        ),
        in_specs=[smem, smem, hbm, vmem, vmem, vmem, vmem],
        out_specs=(hbm, vmem),
        scratch_shapes=[
            [pltpu.VMEM((size, levels * slots, LANES), jnp.float32) for size in SIZES],
            pltpu.VMEM((tiles, levels * number, LANES), jnp.float32),
            pltpu.VMEM((levels * levs, largest), jnp.float32),
            buffers(waves), buffers(waves), buffers(levs, per), buffers(levs, per),
            flat, flat,
            dma((tiles,)), dma((tiles,)), dma((n, waves)), dma((n, waves)),
            dma((n, levs)), dma((n, levs)), dma((n, levs)), dma((n, levs)),
        ],
        compiler_params=pltpu.CompilerParams(
            collective_id=0, has_side_effects=True, vmem_limit_bytes=60 * 2**20
        ),
        name="helmholtz",
    )(picks, senders, spectral.reshape(levels * slots, width), edge, to_modes, from_modes,
      depth.reshape(-1, 1))
    side = side[:, : levels * rest].reshape(number, levels, rest).transpose(1, 0, 2)
    return jnp.concatenate([body.reshape(levels, number, tiles * LANES), side], axis=2)


def solution(mesh):
    placed = (P("lev", "wave", None), P(), P(), P(), P())
    step = functools.partial(per_device, mesh.shape["wave"], mesh.shape["lev"])
    return jax.shard_map(
        step, mesh=mesh, in_specs=placed, out_specs=P("lev", "wave", None), check_vma=False
    )
```

```python
import functools

import jax
import jax.numpy as jnp
from jax import lax
from jax.experimental import pallas as pl
from jax.experimental.pallas import tpu as pltpu
from jax.sharding import PartitionSpec as P

NT = 1279
PLEN = NT + 2
LANES = 128
SPANS = ((0, 8), (16, 4), (8, 8))
EDGE = 1
SPREAD = 4
HALVES = 2
MESH = pl.DeviceIdType.MESH


def rows_of(levels, tiles, rest):
    return -(-(levels * tiles + (rest > 0)) // 8) * 8


def kernel(
    waves, levs, number, levels, slots, rest, chunks,
    owner, spectral, border, to_modes, from_modes, depth, out,
    picks, pairs, held, edge, result, matrix, packs, lands, picked, blocks, backs, homes,
    in_sem, out_sem, send1, recv1, send2, recv2, send3, recv3, send4, recv4,
):
    me = lax.axis_index("wave")
    lev = lax.axis_index("lev")
    per = number // levs
    planes = waves // SPREAD
    n = len(chunks)
    early = n - 1
    sub = chunks[early][1] // HALVES
    lane = lax.rem(lev, 2) * 2 + lax.rem(lev // 2, 2)
    half = lev // SPREAD

    def solver(place, h):
        return (h * 2 + lax.rem(place, 2)) * 2 + place // 2

    def load(c, t):
        at = chunks[c][0] + t
        return pltpu.make_async_copy(
            spectral.at[:, pl.ds(at * LANES, LANES)], held[c].at[t], in_sem.at[at]
        )

    def each_tile(c, act):
        for t in range(chunks[c][1]):
            act(c, t)

    def each_wave(act):
        pl.loop(1, waves)(lambda k: act(lax.rem(me + k, waves)))

    def each_lev(act):
        pl.loop(1, levs)(lambda k: act(lax.rem(lev + k, levs)))

    def each_far(act):
        @pl.loop(0, planes * levs)
        def _(k):
            plane = lax.rem(me // SPREAD + 3 * k, planes)
            b = lax.rem(half * SPREAD + lax.rem(me, SPREAD) + k // planes, levs)
            away = jnp.logical_or(b != lev, plane * SPREAD + lane != me)
            pl.when(away)(lambda: act(b, plane))

    def each_source(act):
        @pl.loop(0, waves)
        def _(k):
            s = lax.rem(me + k, waves)
            for h in range(HALVES):
                j = solver(lax.rem(me, SPREAD), h)
                pl.when(jnp.logical_or(s != me, lev != j))(lambda h=h, j=j: act(s, h, j))

    def wave_copy(c, peer, at):
        return pltpu.make_async_remote_copy(
            src_ref=packs[c].at[peer], dst_ref=lands[c].at[at],
            send_sem=send1.at[c, peer], recv_sem=recv1.at[c, at],
            device_id={"wave": peer}, device_id_type=MESH,
        )

    def part(ref, at, size):
        return ref.at[pl.ds(pl.multiple_of(at * size, 8), size)]

    def far_copy(b, plane, at):
        return pltpu.make_async_remote_copy(
            src_ref=backs[early].at[b * planes + plane], dst_ref=lands[early].at[at],
            send_sem=send4.at[b * planes + plane], recv_sem=recv4.at[at],
            device_id={"wave": plane * SPREAD + lane, "lev": b}, device_id_type=MESH,
        )

    def modal(c, peer, at):
        source = packs[c] if c == early else picked[c]
        return pltpu.make_async_remote_copy(
            src_ref=source.at[peer], dst_ref=blocks[c].at[at],
            send_sem=send2.at[c, peer], recv_sem=recv2.at[c, at],
            device_id={"lev": peer}, device_id_type=MESH,
        )

    def back(c, peer, at):
        size = per * chunks[c][2]
        return pltpu.make_async_remote_copy(
            src_ref=part(backs[c], peer, size), dst_ref=part(homes[c], at, size),
            send_sem=send3.at[c, peer], recv_sem=recv3.at[c, at],
            device_id={"lev": peer}, device_id_type=MESH,
        )

    def rank():
        def step(d, count):
            hits = jnp.int32(0)
            pair = jnp.int32(0)
            for i in range(number):
                hit = (owner[d * number + i] == me).astype(jnp.int32)
                hits = hits + hit
                pair = pair + hit * (d * number + i)
            picks[d] = jnp.minimum(count, slots - 1)
            pairs[d] = pair
            return count + hits

        lax.fori_loop(0, waves, step, jnp.int32(0))

    def border_rows():
        total = jnp.zeros((slots, LANES), jnp.float32)
        lane = lax.broadcasted_iota(jnp.int32, (slots, LANES), 1)
        for l in range(levels):
            line = jnp.where(lane < rest, border[pl.ds(l * slots, slots), :], 0.0)
            total = total + (pltpu.roll(line, l * rest, 1) if l else line)
        edge[...] = total

    def gather(c):
        tiles = chunks[c][1]

        @pl.loop(0, waves)
        def _(d):
            rows = pl.ds(picks[d], levels, stride=slots)
            if c == early:
                for h in range(HALVES):
                    target = packs[c].at[solver(lax.rem(d, SPREAD), h), d // SPREAD]
                    for t in range(sub):
                        target[pl.ds(t, levels, stride=sub), :] = held[c][h * sub + t, rows, :]
                return
            for t in range(tiles):
                packs[c][d, pl.ds(t, levels, stride=tiles), :] = held[c][t, rows, :]
            if c == EDGE:
                packs[c][d, pl.ds(levels * tiles, 1), :] = edge[pl.ds(picks[d], 1), :]

    def select(c):
        @pl.loop(0, number)
        def _(i):
            picked[c][i // per, lax.rem(i, per)] = lands[c][owner[me * number + i]]

        blocks[c][lev] = picked[c][lev]

    def solve(c):
        start, tiles, size = chunks[c]
        count = per
        if c == early:
            start, tiles, count = start + half * sub, sub, planes
        extra = c == EDGE
        wide = (tiles + extra) * LANES
        row = lax.broadcasted_iota(jnp.int32, (levels, LANES), 0)
        belongs = lax.broadcasted_iota(jnp.int32, (levels, LANES), 1) // rest == row
        first = lax.broadcasted_iota(jnp.int32, (LANES, LANES), 0)
        second = lax.broadcasted_iota(jnp.int32, (LANES, LANES), 1)
        square = (levels * levs, levels * levs)
        diagonal = lax.broadcasted_iota(jnp.int32, square, 0) == lax.broadcasted_iota(
            jnp.int32, square, 1
        )
        factor = jnp.sum(jnp.where(diagonal, depth[...], 0.0), axis=1, keepdims=True)

        def exact(a, b):
            return jnp.dot(
                a, b, precision=lax.Precision.HIGHEST, preferred_element_type=jnp.float32
            )

        @pl.loop(0, count)
        def _(p):
            for b in range(levs):
                rows = pl.ds(b * levels, levels)
                for t in range(tiles):
                    matrix[rows, pl.ds(t * LANES, LANES)] = blocks[c][
                        b, p, pl.ds(t, levels, stride=tiles), :
                    ]
                if extra:
                    line = blocks[c][b, p, pl.ds(levels * tiles, 1), :]
                    matrix[rows, pl.ds(tiles * LANES, LANES)] = jnp.where(belongs, line, 0.0)
            if extra:
                fold = (first % rest == second) & (first < levels * rest)
                edges = pl.ds(tiles * LANES, LANES)
                matrix[:, edges] = exact(matrix[:, edges], fold.astype(jnp.float32))
            modes = exact(to_modes[...], matrix[:, pl.ds(0, wide)])
            column = start * LANES + lax.broadcasted_iota(jnp.int32, (1, wide), 1)
            within = jnp.where(column >= PLEN, column - PLEN, column)
            pair = pairs[p * SPREAD + lane] if c == early else me * number + lev * per + p
            degree = jnp.where(within <= NT - pair, pair + within, within - 1)
            ratio = (degree * (degree + 1)).astype(jnp.float32) / float(NT * (NT + 1))
            scaled = modes / (1.0 + factor * ratio)
            matrix[:, pl.ds(0, wide)] = exact(from_modes[...], scaled)
            if extra:
                spread = (second % rest == first) & (second < levels * rest)
                edges = pl.ds(tiles * LANES, LANES)
                matrix[:, edges] = exact(matrix[:, edges], spread.astype(jnp.float32))
            for b in range(levs):
                rows = pl.ds(b * levels, levels)
                at = b * count + p
                for t in range(tiles):
                    block = matrix[rows, pl.ds(t * LANES, LANES)]
                    if c == early:
                        backs[c][at, pl.ds(t, levels, stride=tiles), :] = block
                    else:
                        backs[c][pl.ds(at * size + t, levels, stride=tiles), :] = block
                if extra:
                    line = jnp.where(belongs, matrix[rows, pl.ds(tiles * LANES, LANES)], 0.0)
                    backs[c][pl.ds(at * size + levels * tiles, 1), :] = jnp.sum(
                        line, axis=0, keepdims=True
                    )

        if c != early:
            own = pl.ds(pl.multiple_of(lev * per * size, 8), per * size)
            homes[c][own] = backs[c][own]

    def unpack(c, h=0):
        start, tiles, size = chunks[c]
        if c == early:
            start, tiles = start + h * sub, sub

        @pl.loop(0, levels)
        def _(l):
            rows = pl.ds(pl.multiple_of(l * number, number), number)
            for t in range(tiles):
                result[rows, pl.ds((start + t) * LANES, LANES)] = homes[c][
                    pl.ds(l * tiles + t, number, stride=size), :
                ]

        if c == EDGE:
            line = homes[c][pl.ds(levels * tiles, number, stride=size), :]
            for l in range(levels):
                turned = pltpu.roll(line, LANES - l * rest, 1) if l else line
                result[pl.ds(l * number, number), pl.ds((start + tiles) * LANES, rest)] = turned[
                    :, :rest
                ]

    for c in (0, early, *range(1, early)):
        each_tile(c, lambda c, t: load(c, t).start())
    barrier = pltpu.get_barrier_semaphore()

    def greet(**where):
        pl.semaphore_signal(barrier, inc=1, device_id=where, device_id_type=MESH)

    each_wave(lambda d: greet(wave=d))
    each_lev(lambda b: greet(lev=b))
    each_far(lambda b, plane: greet(wave=plane * SPREAD + lane, lev=b))
    each_source(lambda s, h, j: greet(wave=s, lev=j))
    rank()
    each_tile(0, lambda c, t: load(c, t).wait())
    gather(0)
    own = (lane == lax.rem(me, SPREAD)).astype(jnp.int32)
    pl.semaphore_wait(barrier, waves + levs - 2 + 2 * (HALVES * waves - own))
    each_wave(lambda d: wave_copy(0, d, me).start())
    lands[0][me] = packs[0][me]

    each_tile(early, lambda c, t: load(c, t).wait())
    gather(early)
    each_lev(lambda b: modal(early, b, lev).start())
    blocks[early][lev] = packs[early][lev]
    border_rows()
    for c in range(1, early):
        each_tile(c, lambda c, t: load(c, t).wait())
        gather(c)
        each_wave(lambda d, c=c: wave_copy(c, d, me).start())
        lands[c][me] = packs[c][me]
    each_lev(lambda b: modal(early, b, b).wait_recv())
    solve(early)
    each_far(lambda b, plane: far_copy(b, plane, me * HALVES + half).start())

    @pl.when(own == 1)
    def _():
        lands[early][me * HALVES + half] = backs[early][lev * planes + me // SPREAD]

    def finish(c):
        each_lev(lambda b: back(c, b, b).wait_recv())
        unpack(c)

    for c in range(early):
        each_wave(lambda d, c=c: wave_copy(c, d, d).wait_recv())
        select(c)
        each_lev(lambda b, c=c: modal(c, b, lev).start())
        if c > 0:
            finish(c - 1)
        each_lev(lambda b, c=c: modal(c, b, b).wait_recv())
        solve(c)
        each_lev(lambda b, c=c: back(c, b, lev).start())
    finish(early - 1)
    each_source(lambda s, h, j: far_copy(lev, 0, s * HALVES + h).wait_recv())
    for h in range(HALVES):

        @pl.loop(0, number)
        def _(i):
            size = chunks[early][2]
            homes[early][pl.ds(pl.multiple_of(i * size, 8), levels * sub)] = lands[early][
                owner[me * number + i] * HALVES + h
            ]

        unpack(early, h)
    copy = pltpu.make_async_copy(result, out, out_sem)
    copy.start()
    for c in range(n):
        each_lev(lambda b, c=c: modal(c, b, b).wait_send())
        if c != early:
            each_wave(lambda d, c=c: wave_copy(c, d, d).wait_send())
            each_lev(lambda b, c=c: back(c, b, b).wait_send())
    each_far(lambda b, plane: far_copy(b, plane, 0).wait_send())
    copy.wait()


def per_device(waves, levs, spectral, to_modes, from_modes, depth, owner):
    levels, slots, width = spectral.shape
    number = owner.shape[0] // waves
    per, planes = number // levs, waves // SPREAD
    tiles, rest = divmod(width, LANES)
    n = len(SPANS)
    early = n - 1
    chunks = [
        (start, size, rows_of(levels, size if c < early else size // HALVES, rest * (c == EDGE)))
        for c, (start, size) in enumerate(SPANS)
    ]
    packed = levels * SPANS[early][1] // HALVES
    largest = max(size + (c == EDGE) for c, (_, size) in enumerate(SPANS)) * LANES

    def buffers(*lead, last=()):
        rows = [r for _, _, r in chunks[:early]]
        shapes = [(*lead, r, LANES) for r in rows] + ([(*last, packed, LANES)] if last else [])
        return [pltpu.VMEM(shape, jnp.float32) for shape in shapes]

    flat = [pltpu.VMEM((number * r, LANES), jnp.float32) for _, _, r in chunks]
    vmem = pl.BlockSpec(memory_space=pltpu.VMEM)
    smem = pl.BlockSpec(memory_space=pltpu.SMEM)
    hbm = pl.BlockSpec(memory_space=pl.ANY)
    dma = pltpu.SemaphoreType.DMA
    whole = spectral.reshape(levels * slots, width)
    result = pl.pallas_call(
        functools.partial(kernel, waves, levs, number, levels, slots, rest, chunks),
        out_shape=jax.ShapeDtypeStruct((levels * number, width), jnp.float32),
        in_specs=[
            smem, hbm, pl.BlockSpec((levels * slots, LANES), lambda i: (0, tiles)), vmem, vmem, vmem,
        ],
        grid=(1,),
        out_specs=hbm,
        scratch_shapes=[
            pltpu.SMEM((waves,), jnp.int32), pltpu.SMEM((waves,), jnp.int32),
            [pltpu.VMEM((size, levels * slots, LANES), jnp.float32) for _, size in SPANS],
            pltpu.VMEM((slots, LANES), jnp.float32),
            pltpu.VMEM((levels * number, width), jnp.float32),
            pltpu.VMEM((levels * levs, largest), jnp.float32),
            buffers(waves, last=(levs, planes)),
            buffers(waves, last=(HALVES * waves,)),
            buffers(levs, per),
            buffers(levs, per, last=(levs, planes)),
            [*flat[:early], pltpu.VMEM((levs * planes, packed, LANES), jnp.float32)],
            flat,
            dma((tiles,)), dma, dma((n, waves)), dma((n, waves)),
            dma((n, levs)), dma((n, levs)), dma((n, levs)), dma((n, levs)),
            dma((levs * planes,)), dma((HALVES * waves,)),
        ],
        compiler_params=pltpu.CompilerParams(
            collective_id=0, has_side_effects=True, vmem_limit_bytes=62 * 2**20
        ),
        name="helmholtz",
    )(owner, whole, whole, to_modes, from_modes, depth.reshape(1, -1))
    return result.reshape(levels, number, width)


def solution(mesh):
    placed = (P("lev", "wave", None), P(), P(), P(), P())
    step = functools.partial(per_device, mesh.shape["wave"], mesh.shape["lev"])
    return jax.shard_map(
        step, mesh=mesh, in_specs=placed, out_specs=P("lev", "wave", None), check_vma=False
    )
```

```python
import functools

import jax
import jax.numpy as jnp
from jax import lax
from jax.experimental import pallas as pl
from jax.experimental.pallas import tpu as pltpu
from jax.sharding import PartitionSpec as P

NT = 1279
PLEN = NT + 2
LANES = 128
SPANS = ((16, 4), (0, 6), (6, 4), (10, 6))
EDGE = 0
SPREAD = 4
HALVES = 2
MESH = pl.DeviceIdType.MESH


def rows_of(levels, tiles, rest):
    return -(-(levels * tiles + (rest > 0)) // 2) * 2


def kernel(
    waves, levs, number, levels, slots, rest, chunks,
    owner, spectral, border, to_modes, from_modes, depth, out,
    picks, pairs, held, edge, result, matrix, packs, lands, picked, blocks, backs, homes,
    in_sem, out_sem, send1, recv1, send2, recv2, send3, recv3, send4, recv4,
):
    me = lax.axis_index("wave")
    lev = lax.axis_index("lev")
    planes = waves // SPREAD
    lines = levs // HALVES
    share = number // lines
    n = len(chunks)
    early = n - 1
    row = lev // HALVES
    side = lax.rem(lev, HALVES)
    lane = (1 - side) * 2 + lax.rem(row, 2)
    half = lev // SPREAD

    def solver(place, h):
        return (h * 2 + lax.rem(place, 2)) * 2 + 1 - place // 2

    def load(c, t):
        at = chunks[c][0] + t
        return pltpu.make_async_copy(
            spectral.at[:, pl.ds(at * LANES, LANES)], held[c].at[t], in_sem.at[at]
        )

    def each_tile(c, act):
        for t in range(HALVES * chunks[c][1]):
            act(c, t)

    def each_wave(act):
        @pl.loop(0, waves)
        def _(k):
            d = lax.rem(me + k, waves)
            for x in range(HALVES):
                pl.when(jnp.logical_or(d != me, side != x))(lambda x=x: act(d, x))

    def each_row(act):
        pl.loop(1, lines)(lambda k: act(lax.rem(row + k, lines)))

    def each_lev(act):
        pl.loop(1, levs)(lambda k: act(lax.rem(lev + k, levs)))

    def each_far(act):
        @pl.loop(0, planes * levs)
        def _(k):
            plane = lax.rem(me // SPREAD + 3 * k, planes)
            b = lax.rem(half * SPREAD + lax.rem(me, SPREAD) + k // planes, levs)
            away = jnp.logical_or(b != lev, plane * SPREAD + lane != me)
            pl.when(away)(lambda: act(b, plane))

    def each_source(act):
        @pl.loop(0, waves)
        def _(k):
            s = lax.rem(me + k, waves)
            for h in range(HALVES):
                j = solver(lax.rem(me, SPREAD), h)
                pl.when(jnp.logical_or(s != me, lev != j))(lambda h=h, j=j: act(s, h, j))

    def wave_copy(c, d, x, at):
        return pltpu.make_async_remote_copy(
            src_ref=packs[c].at[d * HALVES + x], dst_ref=lands[c].at[at],
            send_sem=send1.at[c, d * HALVES + x], recv_sem=recv1.at[c, at],
            device_id={"wave": d, "lev": row * HALVES + x}, device_id_type=MESH,
        )

    def wave_start(c):
        each_wave(lambda d, x: wave_copy(c, d, x, me * HALVES + side).start())
        lands[c][me * HALVES + side] = packs[c][me * HALVES + side]

    def part(ref, at, size):
        return ref.at[pl.ds(pl.multiple_of(at * size, 8), size)]

    def far_copy(b, plane, at):
        return pltpu.make_async_remote_copy(
            src_ref=backs[early].at[b * planes + plane], dst_ref=lands[early].at[at],
            send_sem=send4.at[b * planes + plane], recv_sem=recv4.at[at],
            device_id={"wave": plane * SPREAD + lane, "lev": b}, device_id_type=MESH,
        )

    def spread(peer, at):
        return pltpu.make_async_remote_copy(
            src_ref=packs[early].at[peer], dst_ref=blocks[early].at[at],
            send_sem=send2.at[early, peer], recv_sem=recv2.at[early, at],
            device_id={"lev": peer}, device_id_type=MESH,
        )

    def modal(c, peer, at):
        return pltpu.make_async_remote_copy(
            src_ref=picked[c].at[peer], dst_ref=blocks[c].at[at],
            send_sem=send2.at[c, peer], recv_sem=recv2.at[c, at],
            device_id={"lev": peer * HALVES + side}, device_id_type=MESH,
        )

    def back(c, peer, at):
        size = share * chunks[c][2]
        place = lax.rem(at, HALVES) * lines + at // HALVES
        return pltpu.make_async_remote_copy(
            src_ref=part(backs[c], peer, size), dst_ref=part(homes[c], place, size),
            send_sem=send3.at[c, peer], recv_sem=recv3.at[c, at],
            device_id={"lev": peer}, device_id_type=MESH,
        )

    def rank():
        def step(d, count):
            hits = jnp.int32(0)
            pair = jnp.int32(0)
            for i in range(number):
                hit = (owner[d * number + i] == me).astype(jnp.int32)
                hits = hits + hit
                pair = pair + hit * (d * number + i)
            picks[d] = jnp.minimum(count, slots - 1)
            pairs[d] = pair
            return count + hits

        lax.fori_loop(0, waves, step, jnp.int32(0))

    def border_rows():
        total = jnp.zeros((slots, LANES), jnp.float32)
        lane = lax.broadcasted_iota(jnp.int32, (slots, LANES), 1)
        for l in range(levels):
            line = jnp.where(lane < rest, border[pl.ds(l * slots, slots), :], 0.0)
            total = total + (pltpu.roll(line, l * rest, 1) if l else line)
        edge[...] = total

    def gather(c):
        sub = chunks[c][1]

        @pl.loop(0, waves)
        def _(d):
            rows = pl.ds(picks[d], levels, stride=slots)
            for h in range(HALVES):
                if c == early:
                    target = packs[c].at[solver(lax.rem(d, SPREAD), h), d // SPREAD]
                else:
                    target = packs[c].at[d * HALVES + h]
                for t in range(sub):
                    target[pl.ds(t, levels, stride=sub), :] = held[c][h * sub + t, rows, :]
                if c == EDGE:
                    target[pl.ds(levels * sub, 1), :] = edge[pl.ds(picks[d], 1), :]

    def select(c):
        @pl.loop(0, number)
        def _(i):
            for x in range(HALVES):
                picked[c][i // share, x * share + lax.rem(i, share)] = lands[c][
                    owner[me * number + i] * HALVES + x
                ]

        blocks[c][row] = picked[c][row]

    def solve(c):
        start, tiles, size = chunks[c]
        start = start + (half if c == early else side) * tiles
        count = planes if c == early else share
        edge_start = (chunks[EDGE][0] + (HALVES - 1) * chunks[EDGE][1]) * LANES
        extra = c == EDGE
        wide = (tiles + extra) * LANES
        level = lax.broadcasted_iota(jnp.int32, (levels, LANES), 0)
        belongs = lax.broadcasted_iota(jnp.int32, (levels, LANES), 1) // rest == level
        first = lax.broadcasted_iota(jnp.int32, (LANES, LANES), 0)
        second = lax.broadcasted_iota(jnp.int32, (LANES, LANES), 1)
        square = (levels * levs, levels * levs)
        diagonal = lax.broadcasted_iota(jnp.int32, square, 0) == lax.broadcasted_iota(
            jnp.int32, square, 1
        )
        factor = jnp.sum(jnp.where(diagonal, depth[...], 0.0), axis=1, keepdims=True)

        def exact(a, b):
            return jnp.dot(
                a, b, precision=lax.Precision.HIGHEST, preferred_element_type=jnp.float32
            )

        @pl.loop(0, count)
        def _(p):
            for b in range(levs):
                rows = pl.ds(b * levels, levels)
                block = blocks[c].at[b, p]
                if c != early:
                    block = blocks[c].at[b // HALVES, b % HALVES * share + p]
                for t in range(tiles):
                    matrix[rows, pl.ds(t * LANES, LANES)] = block[
                        pl.ds(t, levels, stride=tiles), :
                    ]
                if extra:
                    line = block[pl.ds(levels * tiles, 1), :]
                    matrix[rows, pl.ds(tiles * LANES, LANES)] = jnp.where(belongs, line, 0.0)
            if extra:
                fold = (first % rest == second) & (first < levels * rest)
                edges = pl.ds(tiles * LANES, LANES)
                matrix[:, edges] = exact(matrix[:, edges], fold.astype(jnp.float32))
            modes = exact(to_modes[...], matrix[:, pl.ds(0, wide)])
            column = lax.broadcasted_iota(jnp.int32, (1, wide), 1)
            column = jnp.where(column < tiles * LANES, start * LANES, edge_start) + column
            within = jnp.where(column >= PLEN, column - PLEN, column)
            pair = pairs[p * SPREAD + lane] if c == early else me * number + row * share + p
            degree = jnp.where(within <= NT - pair, pair + within, within - 1)
            ratio = (degree * (degree + 1)).astype(jnp.float32) / float(NT * (NT + 1))
            scaled = modes / (1.0 + factor * ratio)
            matrix[:, pl.ds(0, wide)] = exact(from_modes[...], scaled)
            if extra:
                unfold = (second % rest == first) & (second < levels * rest)
                edges = pl.ds(tiles * LANES, LANES)
                matrix[:, edges] = exact(matrix[:, edges], unfold.astype(jnp.float32))
            for b in range(levs):
                rows = pl.ds(b * levels, levels)
                at = b * count + p
                for t in range(tiles):
                    block = matrix[rows, pl.ds(t * LANES, LANES)]
                    if c == early:
                        backs[c][at, pl.ds(t, levels, stride=tiles), :] = block
                    else:
                        backs[c][pl.ds(at * size + t, levels, stride=tiles), :] = block
                if extra:
                    line = jnp.where(belongs, matrix[rows, pl.ds(tiles * LANES, LANES)], 0.0)
                    backs[c][pl.ds(at * size + levels * tiles, 1), :] = jnp.sum(
                        line, axis=0, keepdims=True
                    )

        if c != early:
            area = share * size
            place = pl.multiple_of((side * lines + row) * area, 8)
            homes[c][pl.ds(place, area)] = backs[c][pl.ds(pl.multiple_of(lev * area, 8), area)]

    def unpack(c, h, offset):
        start, tiles, size = chunks[c]
        start = start + h * tiles

        @pl.loop(0, levels)
        def _(l):
            rows = pl.ds(pl.multiple_of(l * number, number), number)
            for t in range(tiles):
                result[rows, pl.ds((start + t) * LANES, LANES)] = homes[c][
                    pl.ds(offset + l * tiles + t, number, stride=size), :
                ]

        if c == EDGE and h == HALVES - 1:
            line = homes[c][pl.ds(offset + levels * tiles, number, stride=size), :]
            for l in range(levels):
                turned = pltpu.roll(line, LANES - l * rest, 1) if l else line
                result[pl.ds(l * number, number), pl.ds((start + tiles) * LANES, rest)] = turned[
                    :, :rest
                ]

    for c in (0, early, *range(1, early)):
        each_tile(c, lambda c, t: load(c, t).start())
    barrier = pltpu.get_barrier_semaphore()

    def greet(**where):
        pl.semaphore_signal(barrier, inc=1, device_id=where, device_id_type=MESH)

    each_wave(lambda d, x: greet(wave=d, lev=row * HALVES + x))
    each_lev(lambda b: greet(lev=b))
    each_far(lambda b, plane: greet(wave=plane * SPREAD + lane, lev=b))
    each_source(lambda s, h, j: greet(wave=s, lev=j))
    rank()
    border_rows()
    each_tile(0, lambda c, t: load(c, t).wait())
    gather(0)
    own = (lane == lax.rem(me, SPREAD)).astype(jnp.int32)
    pl.semaphore_wait(barrier, HALVES * waves + levs - 2 + 2 * (HALVES * waves - own))
    wave_start(0)

    each_tile(early, lambda c, t: load(c, t).wait())
    gather(early)
    each_lev(lambda b: spread(b, lev).start())
    blocks[early][lev] = packs[early][lev]
    for c in range(1, early):
        each_tile(c, lambda c, t: load(c, t).wait())
        gather(c)
        wave_start(c)
    each_lev(lambda b: spread(b, b).wait_recv())
    solve(early)
    each_far(lambda b, plane: far_copy(b, plane, me * HALVES + half).start())

    @pl.when(own == 1)
    def _():
        lands[early][me * HALVES + half] = backs[early][lev * planes + me // SPREAD]

    def finish(c):
        each_lev(lambda b: back(c, b, b).wait_recv())
        for h in range(HALVES):
            unpack(c, h, h * number * chunks[c][2])

    for c in range(early):
        each_wave(lambda d, x, c=c: wave_copy(c, d, x, d * HALVES + x).wait_recv())
        select(c)
        each_row(lambda r, c=c: modal(c, r, row).start())
        if c > 0:
            finish(c - 1)
        each_row(lambda r, c=c: modal(c, r, r).wait_recv())
        solve(c)
        each_lev(lambda b, c=c: back(c, b, lev).start())
    finish(early - 1)
    each_source(lambda s, h, j: far_copy(lev, 0, s * HALVES + h).wait_recv())
    for h in range(HALVES):

        @pl.loop(0, number)
        def _(i):
            size = chunks[early][2]
            homes[early][pl.ds(i * size, size)] = lands[early][
                owner[me * number + i] * HALVES + h
            ]

        unpack(early, h, 0)
    copy = pltpu.make_async_copy(result, out, out_sem)
    copy.start()
    for c in range(early):
        each_wave(lambda d, x, c=c: wave_copy(c, d, x, 0).wait_send())
        each_row(lambda r, c=c: modal(c, r, r).wait_send())
        each_lev(lambda b, c=c: back(c, b, b).wait_send())
    each_lev(lambda b: spread(b, b).wait_send())
    each_far(lambda b, plane: far_copy(b, plane, 0).wait_send())
    copy.wait()


def per_device(waves, levs, spectral, to_modes, from_modes, depth, owner):
    levels, slots, width = spectral.shape
    number = owner.shape[0] // waves
    planes, lines = waves // SPREAD, levs // HALVES
    share = number // lines
    tiles, rest = divmod(width, LANES)
    n = len(SPANS)
    early = n - 1
    chunks = [
        (start, size // HALVES, rows_of(levels, size // HALVES, rest * (c == EDGE)))
        for c, (start, size) in enumerate(SPANS)
    ]
    largest = max(size + (c == EDGE) for c, (_, size, _) in enumerate(chunks)) * LANES

    def buffers(*lead, last=()):
        shapes = [(*lead, r, LANES) for _, _, r in chunks[:early]]
        shapes += [(*last, chunks[early][2], LANES)] if last else []
        return [pltpu.VMEM(shape, jnp.float32) for shape in shapes]

    flat = [pltpu.VMEM((HALVES * number * r, LANES), jnp.float32) for _, _, r in chunks]
    vmem = pl.BlockSpec(memory_space=pltpu.VMEM)
    smem = pl.BlockSpec(memory_space=pltpu.SMEM)
    hbm = pl.BlockSpec(memory_space=pl.ANY)
    dma = pltpu.SemaphoreType.DMA
    whole = spectral.reshape(levels * slots, width)
    result = pl.pallas_call(
        functools.partial(kernel, waves, levs, number, levels, slots, rest, chunks),
        out_shape=jax.ShapeDtypeStruct((levels * number, width), jnp.float32),
        in_specs=[
            smem, hbm, pl.BlockSpec((levels * slots, LANES), lambda i: (0, tiles)), vmem, vmem, vmem,
        ],
        grid=(1,),
        out_specs=hbm,
        scratch_shapes=[
            pltpu.SMEM((waves,), jnp.int32), pltpu.SMEM((waves,), jnp.int32),
            [pltpu.VMEM((size, levels * slots, LANES), jnp.float32) for _, size in SPANS],
            pltpu.VMEM((slots, LANES), jnp.float32),
            pltpu.VMEM((levels * number, width), jnp.float32),
            pltpu.VMEM((levels * levs, largest), jnp.float32),
            buffers(HALVES * waves, last=(levs, planes)),
            buffers(HALVES * waves, last=(HALVES * waves,)),
            buffers(lines, HALVES * share),
            buffers(lines, HALVES * share, last=(levs, planes)),
            [*flat[:early], *buffers(last=(levs * planes,))[early:]],
            flat,
            dma((tiles,)), dma,
            dma((early, HALVES * waves)), dma((early, HALVES * waves)),
            dma((n, levs)), dma((n, levs)), dma((n, levs)), dma((n, levs)),
            dma((levs * planes,)), dma((HALVES * waves,)),
        ],
        compiler_params=pltpu.CompilerParams(
            collective_id=0, has_side_effects=True, vmem_limit_bytes=62 * 2**20
        ),
        name="helmholtz",
    )(owner, whole, whole, to_modes, from_modes, depth.reshape(1, -1))
    return result.reshape(levels, number, width)


def solution(mesh):
    placed = (P("lev", "wave", None), P(), P(), P(), P())
    step = functools.partial(per_device, mesh.shape["wave"], mesh.shape["lev"])
    return jax.shard_map(
        step, mesh=mesh, in_specs=placed, out_specs=P("lev", "wave", None), check_vma=False
    )
```

```python
import functools

import jax
import jax.numpy as jnp
from jax import lax
from jax.experimental import pallas as pl
from jax.experimental.pallas import tpu as pltpu
from jax.sharding import PartitionSpec as P

NT = 1279
PLEN = NT + 2
LANES = 128
SPANS = ((16, 4), (0, 6), (6, 4), (10, 6))
EDGE = 0
SPREAD = 4
HALVES = 2
MESH = pl.DeviceIdType.MESH


def rows_of(levels, tiles, rest):
    return -(-(levels * tiles + (rest > 0)) // 2) * 2


def kernel(
    waves, levs, number, levels, slots, rest, chunks,
    owner, spectral, border, to_modes, from_modes, depth, out,
    picks, pairs, held, edge, result, matrix, packs, lands, picked, blocks, backs, homes,
    in_sem, out_sem, send1, recv1, send2, recv2, send3, recv3, send4, recv4, entered,
):
    me = lax.axis_index("wave")
    lev = lax.axis_index("lev")
    planes = waves // SPREAD
    lines = levs // HALVES
    share = number // lines
    n = len(chunks)
    early = n - 1
    row = lev // HALVES
    side = lax.rem(lev, HALVES)
    lane = (1 - side) * 2 + lax.rem(row, 2)
    half = lev // SPREAD

    def solver(place, h):
        return (h * 2 + lax.rem(place, 2)) * 2 + 1 - place // 2

    def load(c, t):
        at = chunks[c][0] + t
        return pltpu.make_async_copy(
            spectral.at[:, pl.ds(at * LANES, LANES)], held[c].at[t], in_sem.at[at]
        )

    def each_tile(c, act):
        for t in range(HALVES * chunks[c][1]):
            act(c, t)

    def each_wave(act):
        @pl.loop(0, waves)
        def _(k):
            d = lax.rem(me + k, waves)
            for x in range(HALVES):
                pl.when(jnp.logical_or(d != me, side != x))(lambda x=x: act(d, x))

    def each_row(act):
        pl.loop(1, lines)(lambda k: act(lax.rem(row + k, lines)))

    def each_lev(act):
        pl.loop(1, levs)(lambda k: act(lax.rem(lev + k, levs)))

    def each_far(act):
        @pl.loop(0, planes * levs)
        def _(k):
            plane = lax.rem(me // SPREAD + 3 * k, planes)
            b = lax.rem(half * SPREAD + lax.rem(me, SPREAD) + k // planes, levs)
            away = jnp.logical_or(b != lev, plane * SPREAD + lane != me)
            pl.when(away)(lambda: act(b, plane))

    def each_source(act):
        @pl.loop(0, waves)
        def _(k):
            s = lax.rem(me + k, waves)
            for h in range(HALVES):
                j = solver(lax.rem(me, SPREAD), h)
                pl.when(jnp.logical_or(s != me, lev != j))(lambda h=h, j=j: act(s, h, j))

    def wave_copy(c, d, x, at):
        return pltpu.make_async_remote_copy(
            src_ref=packs[c].at[d * HALVES + x], dst_ref=lands[c].at[at],
            send_sem=send1.at[c, d * HALVES + x], recv_sem=recv1.at[c, at],
            device_id={"wave": d, "lev": row * HALVES + x}, device_id_type=MESH,
        )

    def wave_start(c):
        each_wave(lambda d, x: wave_copy(c, d, x, me * HALVES + side).start())
        lands[c][me * HALVES + side] = packs[c][me * HALVES + side]

    def part(ref, at, size):
        return ref.at[pl.ds(pl.multiple_of(at * size, 8), size)]

    def far_copy(b, plane, at):
        return pltpu.make_async_remote_copy(
            src_ref=backs[early].at[b * planes + plane], dst_ref=lands[early].at[at],
            send_sem=send4.at[b * planes + plane], recv_sem=recv4.at[at],
            device_id={"wave": plane * SPREAD + lane, "lev": b}, device_id_type=MESH,
        )

    def spread(peer, at):
        return pltpu.make_async_remote_copy(
            src_ref=packs[early].at[peer], dst_ref=blocks[early].at[at],
            send_sem=send2.at[early, peer], recv_sem=recv2.at[early, at],
            device_id={"lev": peer}, device_id_type=MESH,
        )

    def modal(c, peer, at):
        return pltpu.make_async_remote_copy(
            src_ref=picked[c].at[peer], dst_ref=blocks[c].at[at],
            send_sem=send2.at[c, peer], recv_sem=recv2.at[c, at],
            device_id={"lev": peer * HALVES + side}, device_id_type=MESH,
        )

    def back(c, peer, at):
        size = share * chunks[c][2]
        place = lax.rem(at, HALVES) * lines + at // HALVES
        return pltpu.make_async_remote_copy(
            src_ref=part(backs[c], peer, size), dst_ref=part(homes[c], place, size),
            send_sem=send3.at[c, peer], recv_sem=recv3.at[c, at],
            device_id={"lev": peer}, device_id_type=MESH,
        )

    def rank():
        def step(d, count):
            hits = jnp.int32(0)
            pair = jnp.int32(0)
            for i in range(number):
                hit = (owner[d * number + i] == me).astype(jnp.int32)
                hits = hits + hit
                pair = pair + hit * (d * number + i)
            picks[d] = jnp.minimum(count, slots - 1)
            pairs[d] = pair
            return count + hits

        lax.fori_loop(0, waves, step, jnp.int32(0))

    def border_rows():
        total = jnp.zeros((slots, LANES), jnp.float32)
        lane = lax.broadcasted_iota(jnp.int32, (slots, LANES), 1)
        for l in range(levels):
            line = jnp.where(lane < rest, border[pl.ds(l * slots, slots), :], 0.0)
            total = total + (pltpu.roll(line, l * rest, 1) if l else line)
        edge[...] = total

    def gather(c):
        sub = chunks[c][1]

        @pl.loop(0, waves)
        def _(d):
            rows = pl.ds(picks[d], levels, stride=slots)
            for h in range(HALVES):
                if c == early:
                    target = packs[c].at[solver(lax.rem(d, SPREAD), h), d // SPREAD]
                else:
                    target = packs[c].at[d * HALVES + h]
                for t in range(sub):
                    target[pl.ds(t, levels, stride=sub), :] = held[c][h * sub + t, rows, :]
                if c == EDGE:
                    target[pl.ds(levels * sub, 1), :] = edge[pl.ds(picks[d], 1), :]

    def select(c):
        @pl.loop(0, number)
        def _(i):
            for x in range(HALVES):
                picked[c][i // share, x * share + lax.rem(i, share)] = lands[c][
                    owner[me * number + i] * HALVES + x
                ]

        blocks[c][row] = picked[c][row]

    def solve(c):
        start, tiles, size = chunks[c]
        start = start + (half if c == early else side) * tiles
        count = planes if c == early else share
        edge_start = (chunks[EDGE][0] + (HALVES - 1) * chunks[EDGE][1]) * LANES
        extra = c == EDGE
        wide = (tiles + extra) * LANES
        level = lax.broadcasted_iota(jnp.int32, (levels, LANES), 0)
        belongs = lax.broadcasted_iota(jnp.int32, (levels, LANES), 1) // rest == level
        first = lax.broadcasted_iota(jnp.int32, (LANES, LANES), 0)
        second = lax.broadcasted_iota(jnp.int32, (LANES, LANES), 1)
        square = (levels * levs, levels * levs)
        diagonal = lax.broadcasted_iota(jnp.int32, square, 0) == lax.broadcasted_iota(
            jnp.int32, square, 1
        )
        factor = jnp.sum(jnp.where(diagonal, depth[...], 0.0), axis=1, keepdims=True)

        def exact(a, b):
            return jnp.dot(
                a, b, precision=lax.Precision.HIGHEST, preferred_element_type=jnp.float32
            )

        @pl.loop(0, count)
        def _(p):
            for b in range(levs):
                rows = pl.ds(b * levels, levels)
                block = blocks[c].at[b, p]
                if c != early:
                    block = blocks[c].at[b // HALVES, b % HALVES * share + p]
                for t in range(tiles):
                    matrix[rows, pl.ds(t * LANES, LANES)] = block[
                        pl.ds(t, levels, stride=tiles), :
                    ]
                if extra:
                    line = block[pl.ds(levels * tiles, 1), :]
                    matrix[rows, pl.ds(tiles * LANES, LANES)] = jnp.where(belongs, line, 0.0)
            if extra:
                fold = (first % rest == second) & (first < levels * rest)
                edges = pl.ds(tiles * LANES, LANES)
                matrix[:, edges] = exact(matrix[:, edges], fold.astype(jnp.float32))
            modes = exact(to_modes[...], matrix[:, pl.ds(0, wide)])
            column = lax.broadcasted_iota(jnp.int32, (1, wide), 1)
            column = jnp.where(column < tiles * LANES, start * LANES, edge_start) + column
            within = jnp.where(column >= PLEN, column - PLEN, column)
            pair = pairs[p * SPREAD + lane] if c == early else me * number + row * share + p
            degree = jnp.where(within <= NT - pair, pair + within, within - 1)
            ratio = (degree * (degree + 1)).astype(jnp.float32) / float(NT * (NT + 1))
            scaled = modes / (1.0 + factor * ratio)
            matrix[:, pl.ds(0, wide)] = exact(from_modes[...], scaled)
            if extra:
                unfold = (second % rest == first) & (second < levels * rest)
                edges = pl.ds(tiles * LANES, LANES)
                matrix[:, edges] = exact(matrix[:, edges], unfold.astype(jnp.float32))
            for b in range(levs):
                rows = pl.ds(b * levels, levels)
                at = b * count + p
                for t in range(tiles):
                    block = matrix[rows, pl.ds(t * LANES, LANES)]
                    if c == early:
                        backs[c][at, pl.ds(t, levels, stride=tiles), :] = block
                    else:
                        backs[c][pl.ds(at * size + t, levels, stride=tiles), :] = block
                if extra:
                    line = jnp.where(belongs, matrix[rows, pl.ds(tiles * LANES, LANES)], 0.0)
                    backs[c][pl.ds(at * size + levels * tiles, 1), :] = jnp.sum(
                        line, axis=0, keepdims=True
                    )

        if c != early:
            area = share * size
            place = pl.multiple_of((side * lines + row) * area, 8)
            homes[c][pl.ds(place, area)] = backs[c][pl.ds(pl.multiple_of(lev * area, 8), area)]

    def unpack(c, h, offset):
        start, tiles, size = chunks[c]
        start = start + h * tiles

        @pl.loop(0, levels)
        def _(l):
            rows = pl.ds(pl.multiple_of(l * number, number), number)
            for t in range(tiles):
                result[rows, pl.ds((start + t) * LANES, LANES)] = homes[c][
                    pl.ds(offset + l * tiles + t, number, stride=size), :
                ]

        if c == EDGE and h == HALVES - 1:
            line = homes[c][pl.ds(offset + levels * tiles, number, stride=size), :]
            for l in range(levels):
                turned = pltpu.roll(line, LANES - l * rest, 1) if l else line
                result[pl.ds(l * number, number), pl.ds((start + tiles) * LANES, rest)] = turned[
                    :, :rest
                ]

    for c in (0, early, *range(1, early)):
        each_tile(c, lambda c, t: load(c, t).start())
    barrier = pltpu.get_barrier_semaphore()

    def greet(**where):
        pl.semaphore_signal(barrier, inc=1, device_id=where, device_id_type=MESH)

    each_wave(lambda d, x: greet(wave=d, lev=row * HALVES + x))
    each_lev(lambda b: greet(lev=b))
    rank()
    border_rows()
    each_tile(0, lambda c, t: load(c, t).wait())
    gather(0)
    own = (lane == lax.rem(me, SPREAD)).astype(jnp.int32)
    pl.semaphore_wait(barrier, HALVES * waves + levs - 2)
    wave_start(0)
    each_lev(
        lambda b: pl.semaphore_signal(entered, inc=1, device_id={"lev": b}, device_id_type=MESH)
    )

    each_tile(early, lambda c, t: load(c, t).wait())
    gather(early)
    each_lev(lambda b: spread(b, lev).start())
    blocks[early][lev] = packs[early][lev]
    for c in range(1, early):
        each_tile(c, lambda c, t: load(c, t).wait())
        gather(c)
        wave_start(c)
    each_lev(lambda b: spread(b, b).wait_recv())
    solve(early)
    pl.semaphore_wait(entered, levs - 1)
    each_far(lambda b, plane: far_copy(b, plane, me * HALVES + half).start())

    @pl.when(own == 1)
    def _():
        lands[early][me * HALVES + half] = backs[early][lev * planes + me // SPREAD]

    def finish(c):
        each_lev(lambda b: back(c, b, b).wait_recv())
        for h in range(HALVES):
            unpack(c, h, h * number * chunks[c][2])

    for c in range(early):
        each_wave(lambda d, x, c=c: wave_copy(c, d, x, d * HALVES + x).wait_recv())
        select(c)
        each_row(lambda r, c=c: modal(c, r, row).start())
        if c > 0:
            finish(c - 1)
        each_row(lambda r, c=c: modal(c, r, r).wait_recv())
        solve(c)
        each_lev(lambda b, c=c: back(c, b, lev).start())
    finish(early - 1)
    each_source(lambda s, h, j: far_copy(lev, 0, s * HALVES + h).wait_recv())
    for h in range(HALVES):

        @pl.loop(0, number)
        def _(i):
            size = chunks[early][2]
            homes[early][pl.ds(i * size, size)] = lands[early][
                owner[me * number + i] * HALVES + h
            ]

        unpack(early, h, 0)
    copy = pltpu.make_async_copy(result, out, out_sem)
    copy.start()
    for c in range(early):
        each_wave(lambda d, x, c=c: wave_copy(c, d, x, 0).wait_send())
        each_row(lambda r, c=c: modal(c, r, r).wait_send())
        each_lev(lambda b, c=c: back(c, b, b).wait_send())
    each_lev(lambda b: spread(b, b).wait_send())
    each_far(lambda b, plane: far_copy(b, plane, 0).wait_send())
    copy.wait()


def per_device(waves, levs, spectral, to_modes, from_modes, depth, owner):
    levels, slots, width = spectral.shape
    number = owner.shape[0] // waves
    planes, lines = waves // SPREAD, levs // HALVES
    share = number // lines
    tiles, rest = divmod(width, LANES)
    n = len(SPANS)
    early = n - 1
    chunks = [
        (start, size // HALVES, rows_of(levels, size // HALVES, rest * (c == EDGE)))
        for c, (start, size) in enumerate(SPANS)
    ]
    largest = max(size + (c == EDGE) for c, (_, size, _) in enumerate(chunks)) * LANES

    def buffers(*lead, last=()):
        shapes = [(*lead, r, LANES) for _, _, r in chunks[:early]]
        shapes += [(*last, chunks[early][2], LANES)] if last else []
        return [pltpu.VMEM(shape, jnp.float32) for shape in shapes]

    flat = [pltpu.VMEM((HALVES * number * r, LANES), jnp.float32) for _, _, r in chunks]
    vmem = pl.BlockSpec(memory_space=pltpu.VMEM)
    smem = pl.BlockSpec(memory_space=pltpu.SMEM)
    hbm = pl.BlockSpec(memory_space=pl.ANY)
    dma = pltpu.SemaphoreType.DMA
    whole = spectral.reshape(levels * slots, width)
    result = pl.pallas_call(
        functools.partial(kernel, waves, levs, number, levels, slots, rest, chunks),
        out_shape=jax.ShapeDtypeStruct((levels * number, width), jnp.float32),
        in_specs=[
            smem, hbm, pl.BlockSpec((levels * slots, LANES), lambda i: (0, tiles)), vmem, vmem, vmem,
        ],
        grid=(1,),
        out_specs=hbm,
        scratch_shapes=[
            pltpu.SMEM((waves,), jnp.int32), pltpu.SMEM((waves,), jnp.int32),
            [pltpu.VMEM((size, levels * slots, LANES), jnp.float32) for _, size in SPANS],
            pltpu.VMEM((slots, LANES), jnp.float32),
            pltpu.VMEM((levels * number, width), jnp.float32),
            pltpu.VMEM((levels * levs, largest), jnp.float32),
            buffers(HALVES * waves, last=(levs, planes)),
            buffers(HALVES * waves, last=(HALVES * waves,)),
            buffers(lines, HALVES * share),
            buffers(lines, HALVES * share, last=(levs, planes)),
            [*flat[:early], *buffers(last=(levs * planes,))[early:]],
            flat,
            dma((tiles,)), dma,
            dma((early, HALVES * waves)), dma((early, HALVES * waves)),
            dma((n, levs)), dma((n, levs)), dma((n, levs)), dma((n, levs)),
            dma((levs * planes,)), dma((HALVES * waves,)),
            pltpu.SemaphoreType.REGULAR,
        ],
        compiler_params=pltpu.CompilerParams(
            collective_id=0, has_side_effects=True, vmem_limit_bytes=62 * 2**20
        ),
        name="helmholtz",
    )(owner, whole, whole, to_modes, from_modes, depth.reshape(1, -1))
    return result.reshape(levels, number, width)


def solution(mesh):
    placed = (P("lev", "wave", None), P(), P(), P(), P())
    step = functools.partial(per_device, mesh.shape["wave"], mesh.shape["lev"])
    return jax.shard_map(
        step, mesh=mesh, in_specs=placed, out_specs=P("lev", "wave", None), check_vma=False
    )
```

```python
import functools

import jax
import jax.numpy as jnp
from jax import lax
from jax.experimental import pallas as pl
from jax.experimental.pallas import tpu as pltpu
from jax.sharding import PartitionSpec as P

NT = 1279
PLEN = NT + 2
LANES = 128
SPANS = ((16, 4), (0, 6), (6, 4), (10, 6))
EDGE = 0
SPREAD = 4
HALVES = 2
MESH = pl.DeviceIdType.MESH


def rows_of(levels, tiles, rest):
    return -(-(levels * tiles + (rest > 0)) // 2) * 2


def kernel(
    waves, levs, number, levels, slots, rest, chunks,
    owner, spectral, border, to_modes, from_modes, depth, out,
    picks, pairs, held, edge, result, matrix, packs, lands, picked, blocks, backs, homes,
    in_sem, out_sem, send1, recv1, send2, recv2, send3, recv3, send4, recv4, entered,
):
    me = lax.axis_index("wave")
    lev = lax.axis_index("lev")
    planes = waves // SPREAD
    lines = levs // HALVES
    share = number // lines
    n = len(chunks)
    early = n - 1
    row = lev // HALVES
    side = lax.rem(lev, HALVES)
    lane = (1 - side) * 2 + lax.rem(row, 2)
    half = lev // SPREAD

    def solver(place, h):
        return (h * 2 + lax.rem(place, 2)) * 2 + 1 - place // 2

    def load(c, t):
        at = chunks[c][0] + t
        return pltpu.make_async_copy(
            spectral.at[:, pl.ds(at * LANES, LANES)], held[c].at[t], in_sem.at[at]
        )

    def each_tile(c, act):
        for t in range(HALVES * chunks[c][1]):
            act(c, t)

    def each_wave(act):
        @pl.loop(0, waves)
        def _(k):
            d = lax.rem(me + 13 * k, waves)
            for x in range(HALVES):
                pl.when(jnp.logical_or(d != me, side != x))(lambda x=x: act(d, x))

    def each_row(act):
        pl.loop(1, lines)(lambda k: act(lax.rem(row + k, lines)))

    def each_lev(act):
        pl.loop(1, levs)(lambda k: act(lax.rem(lev + k, levs)))

    def each_far(act):
        @pl.loop(0, planes * levs)
        def _(k):
            plane = lax.rem(me // SPREAD + 3 * k, planes)
            b = lax.rem(half * SPREAD + lax.rem(me, SPREAD) + k // planes, levs)
            away = jnp.logical_or(b != lev, plane * SPREAD + lane != me)
            pl.when(away)(lambda: act(b, plane))

    def each_source(act):
        @pl.loop(0, waves)
        def _(k):
            s = lax.rem(me + k, waves)
            for h in range(HALVES):
                j = solver(lax.rem(me, SPREAD), h)
                pl.when(jnp.logical_or(s != me, lev != j))(lambda h=h, j=j: act(s, h, j))

    def wave_copy(c, d, x, at):
        return pltpu.make_async_remote_copy(
            src_ref=packs[c].at[d * HALVES + x], dst_ref=lands[c].at[at],
            send_sem=send1.at[c, d * HALVES + x], recv_sem=recv1.at[c, at],
            device_id={"wave": d, "lev": row * HALVES + x}, device_id_type=MESH,
        )

    def wave_start(c):
        each_wave(lambda d, x: wave_copy(c, d, x, me * HALVES + side).start())
        lands[c][me * HALVES + side] = packs[c][me * HALVES + side]

    def part(ref, at, size):
        return ref.at[pl.ds(pl.multiple_of(at * size, 8), size)]

    def far_copy(b, plane, at):
        return pltpu.make_async_remote_copy(
            src_ref=backs[early].at[b * planes + plane], dst_ref=lands[early].at[at],
            send_sem=send4.at[b * planes + plane], recv_sem=recv4.at[at],
            device_id={"wave": plane * SPREAD + lane, "lev": b}, device_id_type=MESH,
        )

    def spread(peer, at):
        return pltpu.make_async_remote_copy(
            src_ref=packs[early].at[peer], dst_ref=blocks[early].at[at],
            send_sem=send2.at[early, peer], recv_sem=recv2.at[early, at],
            device_id={"lev": peer}, device_id_type=MESH,
        )

    def modal(c, peer, at):
        return pltpu.make_async_remote_copy(
            src_ref=picked[c].at[peer], dst_ref=blocks[c].at[at],
            send_sem=send2.at[c, peer], recv_sem=recv2.at[c, at],
            device_id={"lev": peer * HALVES + side}, device_id_type=MESH,
        )

    def back(c, peer, at):
        size = share * chunks[c][2]
        place = lax.rem(at, HALVES) * lines + at // HALVES
        return pltpu.make_async_remote_copy(
            src_ref=part(backs[c], peer, size), dst_ref=part(homes[c], place, size),
            send_sem=send3.at[c, peer], recv_sem=recv3.at[c, at],
            device_id={"lev": peer}, device_id_type=MESH,
        )

    def rank():
        def step(d, count):
            hits = jnp.int32(0)
            pair = jnp.int32(0)
            for i in range(number):
                hit = (owner[d * number + i] == me).astype(jnp.int32)
                hits = hits + hit
                pair = pair + hit * (d * number + i)
            picks[d] = jnp.minimum(count, slots - 1)
            pairs[d] = pair
            return count + hits

        lax.fori_loop(0, waves, step, jnp.int32(0))

    def border_rows():
        total = jnp.zeros((slots, LANES), jnp.float32)
        lane = lax.broadcasted_iota(jnp.int32, (slots, LANES), 1)
        for l in range(levels):
            line = jnp.where(lane < rest, border[pl.ds(l * slots, slots), :], 0.0)
            total = total + (pltpu.roll(line, l * rest, 1) if l else line)
        edge[...] = total

    def gather(c):
        sub = chunks[c][1]

        @pl.loop(0, waves)
        def _(d):
            rows = pl.ds(picks[d], levels, stride=slots)
            for h in range(HALVES):
                if c == early:
                    target = packs[c].at[solver(lax.rem(d, SPREAD), h), d // SPREAD]
                else:
                    target = packs[c].at[d * HALVES + h]
                for t in range(sub):
                    target[pl.ds(t, levels, stride=sub), :] = held[c][h * sub + t, rows, :]
                if c == EDGE:
                    target[pl.ds(levels * sub, 1), :] = edge[pl.ds(picks[d], 1), :]

    def select(c):
        @pl.loop(0, number)
        def _(i):
            for x in range(HALVES):
                picked[c][i // share, x * share + lax.rem(i, share)] = lands[c][
                    owner[me * number + i] * HALVES + x
                ]

        blocks[c][row] = picked[c][row]

    def solve(c):
        start, tiles, size = chunks[c]
        start = start + (half if c == early else side) * tiles
        count = planes if c == early else share
        edge_start = (chunks[EDGE][0] + (HALVES - 1) * chunks[EDGE][1]) * LANES
        extra = c == EDGE
        wide = (tiles + extra) * LANES
        level = lax.broadcasted_iota(jnp.int32, (levels, LANES), 0)
        belongs = lax.broadcasted_iota(jnp.int32, (levels, LANES), 1) // rest == level
        first = lax.broadcasted_iota(jnp.int32, (LANES, LANES), 0)
        second = lax.broadcasted_iota(jnp.int32, (LANES, LANES), 1)
        square = (levels * levs, levels * levs)
        diagonal = lax.broadcasted_iota(jnp.int32, square, 0) == lax.broadcasted_iota(
            jnp.int32, square, 1
        )
        factor = jnp.sum(jnp.where(diagonal, depth[...], 0.0), axis=1, keepdims=True)

        def exact(a, b):
            return jnp.dot(
                a, b, precision=lax.Precision.HIGHEST, preferred_element_type=jnp.float32
            )

        @pl.loop(0, count)
        def _(p):
            for b in range(levs):
                rows = pl.ds(b * levels, levels)
                block = blocks[c].at[b, p]
                if c != early:
                    block = blocks[c].at[b // HALVES, b % HALVES * share + p]
                for t in range(tiles):
                    matrix[rows, pl.ds(t * LANES, LANES)] = block[
                        pl.ds(t, levels, stride=tiles), :
                    ]
                if extra:
                    line = block[pl.ds(levels * tiles, 1), :]
                    matrix[rows, pl.ds(tiles * LANES, LANES)] = jnp.where(belongs, line, 0.0)
            if extra:
                fold = (first % rest == second) & (first < levels * rest)
                edges = pl.ds(tiles * LANES, LANES)
                matrix[:, edges] = exact(matrix[:, edges], fold.astype(jnp.float32))
            modes = exact(to_modes[...], matrix[:, pl.ds(0, wide)])
            column = lax.broadcasted_iota(jnp.int32, (1, wide), 1)
            column = jnp.where(column < tiles * LANES, start * LANES, edge_start) + column
            within = jnp.where(column >= PLEN, column - PLEN, column)
            pair = pairs[p * SPREAD + lane] if c == early else me * number + row * share + p
            degree = jnp.where(within <= NT - pair, pair + within, within - 1)
            ratio = (degree * (degree + 1)).astype(jnp.float32) / float(NT * (NT + 1))
            scaled = modes / (1.0 + factor * ratio)
            matrix[:, pl.ds(0, wide)] = exact(from_modes[...], scaled)
            if extra:
                unfold = (second % rest == first) & (second < levels * rest)
                edges = pl.ds(tiles * LANES, LANES)
                matrix[:, edges] = exact(matrix[:, edges], unfold.astype(jnp.float32))
            for b in range(levs):
                rows = pl.ds(b * levels, levels)
                at = b * count + p
                for t in range(tiles):
                    block = matrix[rows, pl.ds(t * LANES, LANES)]
                    if c == early:
                        backs[c][at, pl.ds(t, levels, stride=tiles), :] = block
                    else:
                        backs[c][pl.ds(at * size + t, levels, stride=tiles), :] = block
                if extra:
                    line = jnp.where(belongs, matrix[rows, pl.ds(tiles * LANES, LANES)], 0.0)
                    backs[c][pl.ds(at * size + levels * tiles, 1), :] = jnp.sum(
                        line, axis=0, keepdims=True
                    )

        if c != early:
            area = share * size
            place = pl.multiple_of((side * lines + row) * area, 8)
            homes[c][pl.ds(place, area)] = backs[c][pl.ds(pl.multiple_of(lev * area, 8), area)]

    def unpack(c, h, offset):
        start, tiles, size = chunks[c]
        start = start + h * tiles

        @pl.loop(0, levels)
        def _(l):
            rows = pl.ds(pl.multiple_of(l * number, number), number)
            for t in range(tiles):
                result[rows, pl.ds((start + t) * LANES, LANES)] = homes[c][
                    pl.ds(offset + l * tiles + t, number, stride=size), :
                ]

        if c == EDGE and h == HALVES - 1:
            line = homes[c][pl.ds(offset + levels * tiles, number, stride=size), :]
            for l in range(levels):
                turned = pltpu.roll(line, LANES - l * rest, 1) if l else line
                result[pl.ds(l * number, number), pl.ds((start + tiles) * LANES, rest)] = turned[
                    :, :rest
                ]

    for c in (0, early, *range(1, early)):
        each_tile(c, lambda c, t: load(c, t).start())
    barrier = pltpu.get_barrier_semaphore()

    def greet(**where):
        pl.semaphore_signal(barrier, inc=1, device_id=where, device_id_type=MESH)

    each_wave(lambda d, x: greet(wave=d, lev=row * HALVES + x))
    each_lev(lambda b: greet(lev=b))
    rank()
    border_rows()
    each_tile(0, lambda c, t: load(c, t).wait())
    gather(0)
    own = (lane == lax.rem(me, SPREAD)).astype(jnp.int32)
    pl.semaphore_wait(barrier, HALVES * waves + levs - 2)
    wave_start(0)
    each_lev(
        lambda b: pl.semaphore_signal(entered, inc=1, device_id={"lev": b}, device_id_type=MESH)
    )

    each_tile(early, lambda c, t: load(c, t).wait())
    gather(early)
    each_lev(lambda b: spread(b, lev).start())
    blocks[early][lev] = packs[early][lev]
    for c in range(1, early):
        each_tile(c, lambda c, t: load(c, t).wait())
        gather(c)
        wave_start(c)
    each_lev(lambda b: spread(b, b).wait_recv())
    solve(early)
    pl.semaphore_wait(entered, levs - 1)
    each_far(lambda b, plane: far_copy(b, plane, me * HALVES + half).start())

    @pl.when(own == 1)
    def _():
        lands[early][me * HALVES + half] = backs[early][lev * planes + me // SPREAD]

    def finish(c):
        each_lev(lambda b: back(c, b, b).wait_recv())
        for h in range(HALVES):
            unpack(c, h, h * number * chunks[c][2])

    for c in range(early):
        each_wave(lambda d, x, c=c: wave_copy(c, d, x, d * HALVES + x).wait_recv())
        select(c)
        each_row(lambda r, c=c: modal(c, r, row).start())
        if c > 0:
            finish(c - 1)
        each_row(lambda r, c=c: modal(c, r, r).wait_recv())
        solve(c)
        each_lev(lambda b, c=c: back(c, b, lev).start())
    finish(early - 1)
    each_source(lambda s, h, j: far_copy(lev, 0, s * HALVES + h).wait_recv())
    for h in range(HALVES):

        @pl.loop(0, number)
        def _(i):
            size = chunks[early][2]
            homes[early][pl.ds(i * size, size)] = lands[early][
                owner[me * number + i] * HALVES + h
            ]

        unpack(early, h, 0)
    copy = pltpu.make_async_copy(result, out, out_sem)
    copy.start()
    for c in range(early):
        each_wave(lambda d, x, c=c: wave_copy(c, d, x, 0).wait_send())
        each_row(lambda r, c=c: modal(c, r, r).wait_send())
        each_lev(lambda b, c=c: back(c, b, b).wait_send())
    each_lev(lambda b: spread(b, b).wait_send())
    each_far(lambda b, plane: far_copy(b, plane, 0).wait_send())
    copy.wait()


def per_device(waves, levs, spectral, to_modes, from_modes, depth, owner):
    levels, slots, width = spectral.shape
    number = owner.shape[0] // waves
    planes, lines = waves // SPREAD, levs // HALVES
    share = number // lines
    tiles, rest = divmod(width, LANES)
    n = len(SPANS)
    early = n - 1
    chunks = [
        (start, size // HALVES, rows_of(levels, size // HALVES, rest * (c == EDGE)))
        for c, (start, size) in enumerate(SPANS)
    ]
    largest = max(size + (c == EDGE) for c, (_, size, _) in enumerate(chunks)) * LANES

    def buffers(*lead, last=()):
        shapes = [(*lead, r, LANES) for _, _, r in chunks[:early]]
        shapes += [(*last, chunks[early][2], LANES)] if last else []
        return [pltpu.VMEM(shape, jnp.float32) for shape in shapes]

    flat = [pltpu.VMEM((HALVES * number * r, LANES), jnp.float32) for _, _, r in chunks]
    vmem = pl.BlockSpec(memory_space=pltpu.VMEM)
    smem = pl.BlockSpec(memory_space=pltpu.SMEM)
    hbm = pl.BlockSpec(memory_space=pl.ANY)
    dma = pltpu.SemaphoreType.DMA
    whole = spectral.reshape(levels * slots, width)
    result = pl.pallas_call(
        functools.partial(kernel, waves, levs, number, levels, slots, rest, chunks),
        out_shape=jax.ShapeDtypeStruct((levels * number, width), jnp.float32),
        in_specs=[
            smem, hbm, pl.BlockSpec((levels * slots, LANES), lambda i: (0, tiles)), vmem, vmem, vmem,
        ],
        grid=(1,),
        out_specs=hbm,
        scratch_shapes=[
            pltpu.SMEM((waves,), jnp.int32), pltpu.SMEM((waves,), jnp.int32),
            [pltpu.VMEM((size, levels * slots, LANES), jnp.float32) for _, size in SPANS],
            pltpu.VMEM((slots, LANES), jnp.float32),
            pltpu.VMEM((levels * number, width), jnp.float32),
            pltpu.VMEM((levels * levs, largest), jnp.float32),
            buffers(HALVES * waves, last=(levs, planes)),
            buffers(HALVES * waves, last=(HALVES * waves,)),
            buffers(lines, HALVES * share),
            buffers(lines, HALVES * share, last=(levs, planes)),
            [*flat[:early], *buffers(last=(levs * planes,))[early:]],
            flat,
            dma((tiles,)), dma,
            dma((early, HALVES * waves)), dma((early, HALVES * waves)),
            dma((n, levs)), dma((n, levs)), dma((n, levs)), dma((n, levs)),
            dma((levs * planes,)), dma((HALVES * waves,)),
            pltpu.SemaphoreType.REGULAR,
        ],
        compiler_params=pltpu.CompilerParams(
            collective_id=0, has_side_effects=True, vmem_limit_bytes=62 * 2**20
        ),
        name="helmholtz",
    )(owner, whole, whole, to_modes, from_modes, depth.reshape(1, -1))
    return result.reshape(levels, number, width)


def solution(mesh):
    placed = (P("lev", "wave", None), P(), P(), P(), P())
    step = functools.partial(per_device, mesh.shape["wave"], mesh.shape["lev"])
    return jax.shard_map(
        step, mesh=mesh, in_specs=placed, out_specs=P("lev", "wave", None), check_vma=False
    )
```

```python
import functools

import jax
import jax.numpy as jnp
from jax import lax
from jax.experimental import pallas as pl
from jax.experimental.pallas import tpu as pltpu
from jax.sharding import PartitionSpec as P

NT = 1279
PLEN = NT + 2
LANES = 128
SPANS = ((16, 4), (0, 6), (6, 4), (10, 6))
EDGE = 0
SPREAD = 4
HALVES = 2
MESH = pl.DeviceIdType.MESH


def rows_of(levels, tiles, rest):
    return -(-(levels * tiles + (rest > 0)) // 2) * 2


def kernel(
    waves, levs, number, levels, slots, rest, chunks,
    owner, spectral, border, to_modes, from_modes, depth, out,
    picks, pairs, held, edge, result, matrix, packs, lands, picked, blocks, backs, homes,
    in_sem, out_sem, send1, recv1, send2, recv2, send3, recv3, send4, recv4, entered,
):
    me = lax.axis_index("wave")
    lev = lax.axis_index("lev")
    planes = waves // SPREAD
    lines = levs // HALVES
    share = number // lines
    n = len(chunks)
    early = n - 1
    row = lev // HALVES
    side = lax.rem(lev, HALVES)
    lane = (1 - side) * 2 + lax.rem(row, 2)
    half = lev // SPREAD

    def solver(place, h):
        return (h * 2 + lax.rem(place, 2)) * 2 + 1 - place // 2

    def load(c, t):
        at = chunks[c][0] + t
        return pltpu.make_async_copy(
            spectral.at[:, pl.ds(at * LANES, LANES)], held[c].at[t], in_sem.at[at]
        )

    def each_tile(c, act):
        for t in range(HALVES * chunks[c][1]):
            act(c, t)

    def each_wave(act):
        @pl.loop(0, waves)
        def _(k):
            d = lax.rem(me + 13 * k, waves)
            for x in range(HALVES):
                pl.when(jnp.logical_or(d != me, side != x))(lambda x=x: act(d, x))

    def each_row(act):
        pl.loop(1, lines)(lambda k: act(lax.rem(row + k, lines)))

    def each_lev(act):
        pl.loop(1, levs)(lambda k: act(lax.rem(lev + k, levs)))

    def each_far(act):
        @pl.loop(0, planes * levs)
        def _(k):
            plane = lax.rem(me // SPREAD + 3 * k, planes)
            b = lax.rem(half * SPREAD + lax.rem(me, SPREAD) + k // planes, levs)
            away = jnp.logical_or(b != lev, plane * SPREAD + lane != me)
            pl.when(away)(lambda: act(b, plane))

    def each_source(act):
        @pl.loop(0, waves)
        def _(k):
            s = lax.rem(me + k, waves)
            for h in range(HALVES):
                j = solver(lax.rem(me, SPREAD), h)
                pl.when(jnp.logical_or(s != me, lev != j))(lambda h=h, j=j: act(s, h, j))

    def wave_copy(c, d, x, at):
        return pltpu.make_async_remote_copy(
            src_ref=packs[c].at[d * HALVES + x], dst_ref=lands[c].at[at],
            send_sem=send1.at[c, d * HALVES + x], recv_sem=recv1.at[c, at],
            device_id={"wave": d, "lev": row * HALVES + x}, device_id_type=MESH,
        )

    def wave_start(c):
        each_wave(lambda d, x: wave_copy(c, d, x, me * HALVES + side).start())
        lands[c][me * HALVES + side] = packs[c][me * HALVES + side]

    def part(ref, at, size):
        return ref.at[pl.ds(pl.multiple_of(at * size, 8), size)]

    def far_copy(b, plane, at):
        return pltpu.make_async_remote_copy(
            src_ref=backs[early].at[b * planes + plane], dst_ref=lands[early].at[at],
            send_sem=send4.at[b * planes + plane], recv_sem=recv4.at[at],
            device_id={"wave": plane * SPREAD + lane, "lev": b}, device_id_type=MESH,
        )

    def spread(peer, at):
        return pltpu.make_async_remote_copy(
            src_ref=packs[early].at[peer], dst_ref=blocks[early].at[at],
            send_sem=send2.at[early, peer], recv_sem=recv2.at[early, at],
            device_id={"lev": peer}, device_id_type=MESH,
        )

    def modal(c, peer, at):
        return pltpu.make_async_remote_copy(
            src_ref=picked[c].at[peer], dst_ref=blocks[c].at[at],
            send_sem=send2.at[c, peer], recv_sem=recv2.at[c, at],
            device_id={"lev": peer * HALVES + side}, device_id_type=MESH,
        )

    def back(c, peer, at):
        size = share * chunks[c][2]
        place = lax.rem(at, HALVES) * lines + at // HALVES
        return pltpu.make_async_remote_copy(
            src_ref=part(backs[c], peer, size), dst_ref=part(homes[c], place, size),
            send_sem=send3.at[c, peer], recv_sem=recv3.at[c, at],
            device_id={"lev": peer}, device_id_type=MESH,
        )

    def rank():
        def step(d, count):
            hits = jnp.int32(0)
            pair = jnp.int32(0)
            for i in range(number):
                hit = (owner[d * number + i] == me).astype(jnp.int32)
                hits = hits + hit
                pair = pair + hit * (d * number + i)
            picks[d] = jnp.minimum(count, slots - 1)
            pairs[d] = pair
            return count + hits

        lax.fori_loop(0, waves, step, jnp.int32(0))

    def border_rows():
        total = jnp.zeros((slots, LANES), jnp.float32)
        lane = lax.broadcasted_iota(jnp.int32, (slots, LANES), 1)
        for l in range(levels):
            line = jnp.where(lane < rest, border[pl.ds(l * slots, slots), :], 0.0)
            total = total + (pltpu.roll(line, l * rest, 1) if l else line)
        edge[pl.ds(0, slots), :] = total

    def gather(c):
        sub = chunks[c][1]

        @pl.loop(0, waves)
        def _(d):
            rows = pl.ds(picks[d], levels, stride=slots)
            for h in range(HALVES):
                if c == early:
                    target = packs[c].at[solver(lax.rem(d, SPREAD), h), d // SPREAD]
                else:
                    target = packs[c].at[d * HALVES + h]
                for t in range(sub):
                    target[pl.ds(t, levels, stride=sub), :] = held[c][h * sub + t, rows, :]
                if c == EDGE:
                    target[pl.ds(levels * sub, 1), :] = edge[pl.ds(picks[d], 1), :]

    def select(c):
        @pl.loop(0, number)
        def _(i):
            for x in range(HALVES):
                picked[c][i // share, x * share + lax.rem(i, share)] = lands[c][
                    owner[me * number + i] * HALVES + x
                ]

        blocks[c][row] = picked[c][row]

    def solve(c):
        start, tiles, size = chunks[c]
        start = start + (half if c == early else side) * tiles
        count = planes if c == early else share
        edge_start = (chunks[EDGE][0] + (HALVES - 1) * chunks[EDGE][1]) * LANES
        extra = c == EDGE
        wide = (tiles + extra) * LANES
        level = lax.broadcasted_iota(jnp.int32, (levels, LANES), 0)
        belongs = lax.broadcasted_iota(jnp.int32, (levels, LANES), 1) // rest == level
        first = lax.broadcasted_iota(jnp.int32, (LANES, LANES), 0)
        second = lax.broadcasted_iota(jnp.int32, (LANES, LANES), 1)
        square = (levels * levs, levels * levs)
        diagonal = lax.broadcasted_iota(jnp.int32, square, 0) == lax.broadcasted_iota(
            jnp.int32, square, 1
        )
        factor = jnp.sum(jnp.where(diagonal, depth[...], 0.0), axis=1, keepdims=True)

        def exact(a, b):
            return jnp.dot(
                a, b, precision=lax.Precision.HIGHEST, preferred_element_type=jnp.float32
            )

        @pl.loop(0, count)
        def _(p):
            for b in range(levs):
                rows = pl.ds(b * levels, levels)
                block = blocks[c].at[b, p]
                if c != early:
                    block = blocks[c].at[b // HALVES, b % HALVES * share + p]
                for t in range(tiles):
                    matrix[rows, pl.ds(t * LANES, LANES)] = block[
                        pl.ds(t, levels, stride=tiles), :
                    ]
                if extra:
                    line = block[pl.ds(levels * tiles, 1), :]
                    matrix[rows, pl.ds(tiles * LANES, LANES)] = jnp.where(belongs, line, 0.0)
            if extra:
                fold = (first % rest == second) & (first < levels * rest)
                edges = pl.ds(tiles * LANES, LANES)
                matrix[:, edges] = exact(matrix[:, edges], fold.astype(jnp.float32))
            modes = exact(to_modes[...], matrix[:, pl.ds(0, wide)])
            column = lax.broadcasted_iota(jnp.int32, (1, wide), 1)
            column = jnp.where(column < tiles * LANES, start * LANES, edge_start) + column
            within = jnp.where(column >= PLEN, column - PLEN, column)
            pair = pairs[p * SPREAD + lane] if c == early else me * number + row * share + p
            degree = jnp.where(within <= NT - pair, pair + within, within - 1)
            ratio = (degree * (degree + 1)).astype(jnp.float32) / float(NT * (NT + 1))
            scaled = modes / (1.0 + factor * ratio)
            matrix[:, pl.ds(0, wide)] = exact(from_modes[...], scaled)
            if extra:
                unfold = (second % rest == first) & (second < levels * rest)
                edges = pl.ds(tiles * LANES, LANES)
                matrix[:, edges] = exact(matrix[:, edges], unfold.astype(jnp.float32))
            for b in range(levs):
                rows = pl.ds(b * levels, levels)
                at = b * count + p
                for t in range(tiles):
                    block = matrix[rows, pl.ds(t * LANES, LANES)]
                    if c == early:
                        backs[c][at, pl.ds(t, levels, stride=tiles), :] = block
                    else:
                        backs[c][pl.ds(at * size + t, levels, stride=tiles), :] = block
                if extra:
                    line = jnp.where(belongs, matrix[rows, pl.ds(tiles * LANES, LANES)], 0.0)
                    backs[c][pl.ds(at * size + levels * tiles, 1), :] = jnp.sum(
                        line, axis=0, keepdims=True
                    )

        if c != early:
            area = share * size
            place = pl.multiple_of((side * lines + row) * area, 8)
            homes[c][pl.ds(place, area)] = backs[c][pl.ds(pl.multiple_of(lev * area, 8), area)]

    def unpack(c, h, offset):
        start, tiles, size = chunks[c]
        start = start + h * tiles

        @pl.loop(0, levels)
        def _(l):
            rows = pl.ds(pl.multiple_of(l * number, number), number)
            for t in range(tiles):
                result[rows, pl.ds((start + t) * LANES, LANES)] = homes[c][
                    pl.ds(offset + l * tiles + t, number, stride=size), :
                ]

        if c == EDGE and h == HALVES - 1:
            line = homes[c][pl.ds(offset + levels * tiles, number, stride=size), :]
            for l in range(levels):
                turned = pltpu.roll(line, LANES - l * rest, 1) if l else line
                result[pl.ds(l * number, number), pl.ds((start + tiles) * LANES, rest)] = turned[
                    :, :rest
                ]

    for c in (0, early, *range(1, early)):
        each_tile(c, lambda c, t: load(c, t).start())
    barrier = pltpu.get_barrier_semaphore()

    def greet(**where):
        pl.semaphore_signal(barrier, inc=1, device_id=where, device_id_type=MESH)

    each_wave(lambda d, x: greet(wave=d, lev=row * HALVES + x))
    each_lev(lambda b: greet(lev=b))
    rank()
    border_rows()
    each_tile(0, lambda c, t: load(c, t).wait())
    gather(0)
    own = (lane == lax.rem(me, SPREAD)).astype(jnp.int32)
    pl.semaphore_wait(barrier, HALVES * waves + levs - 2)
    wave_start(0)
    each_lev(
        lambda b: pl.semaphore_signal(entered, inc=1, device_id={"lev": b}, device_id_type=MESH)
    )

    each_tile(early, lambda c, t: load(c, t).wait())
    gather(early)
    each_lev(lambda b: spread(b, lev).start())
    blocks[early][lev] = packs[early][lev]
    for c in range(1, early):
        each_tile(c, lambda c, t: load(c, t).wait())
        gather(c)
        wave_start(c)
    each_lev(lambda b: spread(b, b).wait_recv())
    solve(early)
    pl.semaphore_wait(entered, levs - 1)
    each_far(lambda b, plane: far_copy(b, plane, me * HALVES + half).start())

    @pl.when(own == 1)
    def _():
        lands[early][me * HALVES + half] = backs[early][lev * planes + me // SPREAD]

    def finish(c):
        each_lev(lambda b: back(c, b, b).wait_recv())
        for h in range(HALVES):
            unpack(c, h, h * number * chunks[c][2])

    for c in range(early):
        each_wave(lambda d, x, c=c: wave_copy(c, d, x, d * HALVES + x).wait_recv())
        select(c)
        each_row(lambda r, c=c: modal(c, r, row).start())
        if c > 0:
            finish(c - 1)
        each_row(lambda r, c=c: modal(c, r, r).wait_recv())
        solve(c)
        each_lev(lambda b, c=c: back(c, b, lev).start())
    finish(early - 1)
    each_source(lambda s, h, j: far_copy(lev, 0, s * HALVES + h).wait_recv())
    for h in range(HALVES):

        @pl.loop(0, number)
        def _(i):
            size = chunks[early][2]
            homes[early][pl.ds(i * size, size)] = lands[early][
                owner[me * number + i] * HALVES + h
            ]

        unpack(early, h, 0)
    copy = pltpu.make_async_copy(result, out, out_sem)
    copy.start()
    for c in range(early):
        each_wave(lambda d, x, c=c: wave_copy(c, d, x, 0).wait_send())
        each_row(lambda r, c=c: modal(c, r, r).wait_send())
        each_lev(lambda b, c=c: back(c, b, b).wait_send())
    each_lev(lambda b: spread(b, b).wait_send())
    each_far(lambda b, plane: far_copy(b, plane, 0).wait_send())
    copy.wait()


def per_device(waves, levs, spectral, to_modes, from_modes, depth, owner):
    levels, slots, width = spectral.shape
    number = owner.shape[0] // waves
    planes, lines = waves // SPREAD, levs // HALVES
    share = number // lines
    tiles, rest = divmod(width, LANES)
    n = len(SPANS)
    early = n - 1
    chunks = [
        (start, size // HALVES, rows_of(levels, size // HALVES, rest * (c == EDGE)))
        for c, (start, size) in enumerate(SPANS)
    ]
    largest = max(size + (c == EDGE) for c, (_, size, _) in enumerate(chunks)) * LANES

    def buffers(*lead, last=()):
        shapes = [(*lead, r, LANES) for _, _, r in chunks[:early] if lead]
        shapes += [(*last, chunks[early][2], LANES)] if last else []
        return [pltpu.VMEM((shape[0] + 1, *shape[1:]), jnp.float32) for shape in shapes]

    flat = [pltpu.VMEM((HALVES * number * r + 128, LANES), jnp.float32) for _, _, r in chunks]
    vmem = pl.BlockSpec(memory_space=pltpu.VMEM)
    smem = pl.BlockSpec(memory_space=pltpu.SMEM)
    hbm = pl.BlockSpec(memory_space=pl.ANY)
    dma = pltpu.SemaphoreType.DMA
    whole = spectral.reshape(levels * slots, width)
    result = pl.pallas_call(
        functools.partial(kernel, waves, levs, number, levels, slots, rest, chunks),
        out_shape=jax.ShapeDtypeStruct((levels * number, width), jnp.float32),
        in_specs=[
            smem, hbm, pl.BlockSpec((levels * slots, LANES), lambda i: (0, tiles)), vmem, vmem, vmem,
        ],
        grid=(1,),
        out_specs=hbm,
        scratch_shapes=[
            pltpu.SMEM((waves,), jnp.int32), pltpu.SMEM((waves,), jnp.int32),
            [pltpu.VMEM((size + 1, levels * slots, LANES), jnp.float32) for _, size in SPANS],
            pltpu.VMEM((slots + 8, LANES), jnp.float32),
            pltpu.VMEM((levels * number, width), jnp.float32),
            pltpu.VMEM((levels * levs, largest), jnp.float32),
            buffers(HALVES * waves, last=(levs, planes)),
            buffers(HALVES * waves, last=(HALVES * waves,)),
            buffers(lines, HALVES * share),
            buffers(lines, HALVES * share, last=(levs, planes)),
            [*flat[:early], *buffers(last=(levs * planes,))],
            flat,
            dma((tiles,)), dma,
            dma((early, HALVES * waves)), dma((early, HALVES * waves)),
            dma((n, levs)), dma((n, levs)), dma((n, levs)), dma((n, levs)),
            dma((levs * planes,)), dma((HALVES * waves,)),
            pltpu.SemaphoreType.REGULAR,
        ],
        compiler_params=pltpu.CompilerParams(
            collective_id=0, has_side_effects=True, vmem_limit_bytes=62 * 2**20
        ),
        name="helmholtz",
    )(owner, whole, whole, to_modes, from_modes, depth.reshape(1, -1))
    return result.reshape(levels, number, width)


def solution(mesh):
    placed = (P("lev", "wave", None), P(), P(), P(), P())
    step = functools.partial(per_device, mesh.shape["wave"], mesh.shape["lev"])
    return jax.shard_map(
        step, mesh=mesh, in_specs=placed, out_specs=P("lev", "wave", None), check_vma=False
    )
```
